128 devices in a mesh: rows: 128 (over z, y, x, core).
Axes of the slice: x: 4, y: 4, z: 4, core: 2. Of those that a mesh axis runs over, the one named last changes fastest.
Arguments:
- events: float32 [4, 32, 1048576], P(None, None, 'rows'), may hold values from -8 to 8
- keep_indicator: int32 [4, 1048576], P(None, 'rows'), may hold values from 0 to 1, as said below
Outputs:
- lagging_mean: float32 [4, 32, 1048576], P(None, None, 'rows')
- deviation: float32 [4, 32, 1048576], P(None, None, 'rows')
The draws below stay inside these ranges and needn't reach their ends.
Inputs may be any that keep to these rules, and one draw needn't show every extreme that they name: `keep_indicator`: in each table, each of the 128 aligned blocks of 8192 rows holds at least 4096 survivors, and some block holds exactly 4096.
All inputs are finite; a program needn't handle non-finite values.
Results may differ from the reference program's by a relative error of at most 0.0003.
Values sent between devices are 32-bit elements; how exact they have to be, the bound alone decides.
A program may use at most 128 MiB of HBM per device.

```python
import jax
import jax.numpy as jnp
from jax import lax

COLS = 32
SPAN_LENGTH = 4096
STREAMS = 4
ROWS_DEV = 8192
N_ROWS = 128


def draw_events(key, part):
    noise_key, level_key = jax.random.split(jax.random.fold_in(key, 11), 2)
    shape = (STREAMS, COLS, ROWS_DEV * N_ROWS)
    noise = jax.random.truncated_normal(noise_key, -4.0, 4.0, shape, jnp.float32)
    levels = jax.random.uniform(level_key, (STREAMS, 1, N_ROWS), jnp.float32, -2.0, 2.0)
    levels = jnp.broadcast_to(levels, (STREAMS, COLS, N_ROWS))
    spread = jnp.repeat(levels, ROWS_DEV, axis=2, total_repeat_length=ROWS_DEV * N_ROWS)
    return (noise + spread).astype(jnp.float32)


def draw_keep_indicator(key, part):
    count_key, perm_key, forced_key = jax.random.split(jax.random.fold_in(key, 23), 3)
    draws = jax.random.randint(count_key, (STREAMS, N_ROWS, 2), 0, ROWS_DEV - SPAN_LENGTH + 1)
    keep = SPAN_LENGTH + jnp.min(draws, axis=2)
    forced = jax.random.randint(forced_key, (STREAMS, 1), 0, N_ROWS)
    keep = jnp.where(jnp.arange(N_ROWS)[None, :] == forced, SPAN_LENGTH, keep)
    keys = jax.random.split(perm_key, STREAMS * N_ROWS)
    perms = jax.vmap(lambda single: jax.random.permutation(single, ROWS_DEV))(keys)
    perms = perms.reshape(STREAMS, N_ROWS, ROWS_DEV)
    mask = (perms < keep[:, :, None]).astype(jnp.int32)
    return mask.reshape(STREAMS, N_ROWS * ROWS_DEV)


def setup_inputs(seed: int = 0) -> dict:
    streams_of = jax.random.split(jax.random.key(seed), 3)
    return {
        "events": draw_events(jax.random.fold_in(streams_of[2], 71), 0),
        "keep_indicator": draw_keep_indicator(jax.random.fold_in(streams_of[2], 71), 0),
    }


def single_table_input(pair):
    values, persisting_flags = pair
    feature_width = values.shape[0]
    total_rows = values.shape[1]
    retained_rows = values * persisting_flags[None, :].astype(jnp.float32)
    order = jnp.argsort(1 - persisting_flags, stable=True).astype(jnp.int32)
    packed_entries = jnp.take(retained_rows, order, axis=1)
    extended = jnp.concatenate([jnp.zeros((feature_width, SPAN_LENGTH), jnp.float32), packed_entries], axis=1)
    blocks = extended.reshape(feature_width, (total_rows + SPAN_LENGTH) // SPAN_LENGTH, SPAN_LENGTH)
    partial_sums = jnp.cumsum(blocks, axis=2)
    whole = partial_sums[:, :, -1]
    trailing = partial_sums[:, 1:, :] + (whole[:, :-1, None] - partial_sums[:, :-1, :])
    trailing = trailing.reshape(feature_width, total_rows)
    remaining_position = jnp.cumsum(persisting_flags).astype(jnp.int32)
    gather_slot = jnp.maximum(remaining_position - 1, 0).astype(jnp.int32)
    selected_entries = jnp.take(trailing, gather_slot, axis=1)
    lagging_mean = jnp.where(remaining_position[None, :] >= 1, selected_entries, jnp.float32(0.0)) / SPAN_LENGTH
    local = jnp.cumsum(retained_rows.reshape(feature_width, N_ROWS, ROWS_DEV), axis=2)
    ends = local[:, :, -1]
    starts = jnp.cumsum(ends, axis=1) - ends
    running = (local + starts[:, :, None]).reshape(feature_width, total_rows)
    visited_tally = jnp.maximum(remaining_position.astype(jnp.float32), 1.0)
    deviation = lagging_mean - running / visited_tally[None, :]
    return lagging_mean, deviation


def reference(events, keep_indicator):
    lagging_mean, deviation = lax.map(single_table_input, (events, keep_indicator))
    return (lagging_mean, deviation)
```

```python
import functools

import jax
import jax.numpy as jnp
from jax import lax
from jax.experimental import pallas as pl
from jax.experimental.pallas import tpu as pltpu
from jax.sharding import PartitionSpec as P

SPAN = 4096
W = 128
STREAMS = 4
COLS = 32
ROWS = 8192
TILES = ROWS // W
TABLE = ROWS + 2 * W
EARLY = SPAN + W
MESH = pl.DeviceIdType.MESH
F32 = jnp.float32
I32 = jnp.int32
BF16 = jnp.bfloat16


def lanes_of(shape):
    return lax.broadcasted_iota(I32, shape, len(shape) - 1)


def rows_of(shape):
    return lax.broadcasted_iota(I32, shape, 0)


def lane_gather(values, index):
    return jnp.take_along_axis(values, index, axis=1, mode="promise_in_bounds")


def dot(a, b):
    return jnp.dot(a, b, preferred_element_type=F32)


def make_weights(w_ref):
    r = rows_of(w_ref.shape) % W
    c = lanes_of(w_ref.shape)
    w_ref[...] = ((r <= c % W) | (c >= W)).astype(F32).astype(BF16)


def index_maps(keep_ref, keepf_ref, src_ref, rank_ref, places_ref):
    for t in range(TILES):
        keepf_ref[pl.ds(4 * t, 4), :] = keep_ref[:, t * W : (t + 1) * W].astype(F32)
    keep = keepf_ref[...].astype(BF16)
    tri = (rows_of((W, W)) <= lanes_of((W, W))).astype(F32).astype(BF16)
    ones = jnp.ones((W, W), BF16)
    inside = dot(keep, tri)
    count = dot(keep, ones).astype(BF16)
    n = TILES * STREAMS
    ri, ci = rows_of((n, n)), lanes_of((n, n))
    same = ri % STREAMS == ci % STREAMS
    before = (same & (ci // STREAMS < ri // STREAMS)).astype(F32).astype(BF16)
    after = (same & (ri // STREAMS < ci // STREAMS)).astype(F32).astype(BF16)
    same = same.astype(F32).astype(BF16)
    count_row = lax.dot_general(
        jnp.ones((8, W), BF16), keep, (((1,), (1,)), ((), ())), preferred_element_type=F32
    ).astype(BF16)
    start_row = dot(count_row, after).astype(I32)
    total_row = dot(count_row, same).astype(I32)
    sub = rows_of((8, n))
    places_ref[...] = jnp.where(
        sub == 0, start_row, jnp.where(sub == 1, start_row - total_row + ROWS, total_row)
    )
    start = dot(before, count).astype(I32)
    total = dot(same, count).astype(I32)
    inside = inside.astype(I32)
    rank_ref[...] = start + inside
    offset = (start - total) & (W - 1)
    wanted = (lanes_of((n, W)) - offset) & (W - 1)
    found = jnp.zeros((n, W), I32)
    for step in (64, 32, 16, 8, 4, 2, 1):
        probe = lane_gather(inside, found + (step - 1))
        found = jnp.where(probe <= wanted, found + step, found)
    src_ref[...] = found


def pack(s, events_ref, keepf_ref, src_ref, at, w_ref, table, prefix_ref, tail_ref, early_ref, total_ref):
    lane = lanes_of((COLS, W))
    group = 8

    def body(g, carry):
        base, current = carry
        kept, lhs = [], []
        for u in range(group):
            t = g * group + u
            x = events_ref[0, :, pl.ds(pl.multiple_of(t * W, W), W)]
            x = x * keepf_ref[pl.ds(STREAMS * t + s, 1), :]
            kept.append(x)
            hi = x.astype(BF16)
            rest = x - hi.astype(F32)
            mid = rest.astype(BF16)
            low = (rest - mid.astype(F32)).astype(BF16)
            lhs.append(jnp.concatenate([hi, mid, low], axis=1))
        sums = dot(jnp.concatenate(lhs, axis=0), w_ref[...])
        for u in range(group):
            t = g * group + u
            part = sums[u * COLS : (u + 1) * COLS]
            prefix = base + part[:, :W]
            base = base + part[:, W:]
            prefix_ref[:, pl.ds(pl.multiple_of(t * W, W), W)] = prefix
            index = jnp.broadcast_to(src_ref[pl.ds(STREAMS * t + s, 1), :], (COLS, W))
            moved = lane_gather(prefix - kept[u], index)
            place = at[1, STREAMS * t + s]
            later = jnp.where(t == TILES - 1, ROWS, at[1, jnp.minimum(STREAMS * (t + 1), STREAMS * (TILES - 1)) + s])
            block = place // W
            current = jnp.where(lane >= place % W, moved, current)
            table[:, pl.ds(pl.multiple_of(block * W, W), W)] = current
            current = jnp.where(later // W > block, moved, current)
        return base, current

    zero = jnp.zeros((COLS, W), F32)
    total, _ = lax.fori_loop(0, TILES // group, body, (zero, zero))
    total_ref[...] = total
    for t in range(SPAN // W):
        tail_ref[:, t * W : (t + 1) * W] = table[:, SPAN + t * W : SPAN + (t + 1) * W] - total
    first = ROWS - at[2, s]
    block, shift = first // W, first % W
    turn = (lane + shift) & (W - 1)
    fresh = lane < W - shift

    def rolled(j):
        return lane_gather(table[:, pl.ds(pl.multiple_of((block + j) * W, W), W)], turn)

    def early(g, now):
        for u in range(3):
            j = g * 3 + u
            following = rolled(j + 1)
            early_ref[:, pl.ds(pl.multiple_of(j * W, W), W)] = jnp.where(fresh, now, following)
            now = following
        return now

    lax.fori_loop(0, EARLY // W // 3, early, rolled(0))


def first_kernel(
    keep_ref, events_ref,
    keepf_ref, src_ref, rank_ref, places_ref, prefix_ref, tail_ref, early_ref, total_ref,
    w_ref, table, at, sem,
):
    make_weights(w_ref)
    index_maps(keep_ref, keepf_ref, src_ref, rank_ref, places_ref)
    copy = pltpu.make_async_copy(places_ref, at, sem)
    copy.start()
    copy.wait()
    pack(0, events_ref, keepf_ref, src_ref, at, w_ref, table, prefix_ref, tail_ref, early_ref, total_ref)


def pack_kernel(
    s, at, events_ref, keepf_ref, src_ref,
    prefix_ref, tail_ref, early_ref, total_ref,
    w_ref, table,
):
    make_weights(w_ref)
    pack(s, events_ref, keepf_ref, src_ref, at, w_ref, table, prefix_ref, tail_ref, early_ref, total_ref)


def shape(*dims, dtype=F32):
    return jax.ShapeDtypeStruct(dims, dtype)


VMEM = pl.BlockSpec(memory_space=pltpu.VMEM)
SMEM = pl.BlockSpec(memory_space=pltpu.SMEM)
HBM = pl.BlockSpec(memory_space=pl.ANY)
PACKED = (shape(COLS, ROWS), shape(COLS, SPAN), shape(COLS, EARLY), shape(COLS, W))
PARAMS = pltpu.CompilerParams(vmem_limit_bytes=32 * 2**20)
COST = pl.CostEstimate(flops=2_000_000_000, bytes_accessed=4 * 2**20, transcendentals=0)


def stream_block(s):
    return pl.BlockSpec((1, COLS, ROWS), lambda i: (s, 0, 0))


def whole(*dims):
    return pl.BlockSpec(dims, lambda i: (0,) * len(dims))


def pack_first(events, keep):
    n = TILES * STREAMS
    maps = (shape(n, W), shape(n, W, dtype=I32), shape(n, W, dtype=I32), shape(8, n, dtype=I32))
    outs = maps + PACKED
    return pl.pallas_call(
        first_kernel,
        grid=(1,),
        in_specs=[whole(STREAMS, ROWS), stream_block(0)],
        out_specs=[whole(*o.shape) for o in outs],
        out_shape=outs,
        scratch_shapes=[
            pltpu.VMEM((3 * W, 2 * W), BF16),
            pltpu.VMEM((COLS, TABLE), F32),
            pltpu.SMEM((8, n), I32),
            pltpu.SemaphoreType.DMA,
        ],
        compiler_params=PARAMS,
        cost_estimate=COST,
        name="pack_first",
    )(keep, events)


def pack_stream(s, places, events, keepf, src):
    n = TILES * STREAMS
    return pl.pallas_call(
        functools.partial(pack_kernel, s),
        grid=(1,),
        in_specs=[SMEM, stream_block(s), whole(n, W), whole(n, W)],
        out_specs=[whole(*o.shape) for o in PACKED],
        out_shape=PACKED,
        scratch_shapes=[pltpu.VMEM((3 * W, 2 * W), BF16), pltpu.VMEM((COLS, TABLE), F32)],
        compiler_params=PARAMS,
        cost_estimate=COST,
        name=f"pack_{s}",
    )(places, events, keepf, src)


def scan_kernel(
    places, t0, t1, t2, t3, out_ref,
    mine, half, across, plane, send, result,
    half_sem, across_sem, plane_sem, back_sem, send_sem,
):
    me = lax.axis_index("rows")
    core, chip = me % 2, me // 2
    x, zy = chip % 4, chip // 4
    even = core == 0

    def other_x(step):
        return (zy * 4 + (x + step) % 4) * 2

    def other_plane(step):
        return (((zy + step) % 16) * 4 + x) * 2

    barrier = pltpu.get_barrier_semaphore()

    def greet(device):
        pl.semaphore_signal(barrier, inc=1, device_id=(device,), device_id_type=MESH)

    greet(me + 1 - 2 * core)

    @pl.when(even)
    def _():
        for step in range(1, 4):
            greet(other_x(step))
        for step in range(1, 16):
            greet(other_plane(step))

    lane = lanes_of((8, W))
    message = jnp.zeros((8, W), F32)
    for s, total in enumerate((t0, t1, t2, t3)):
        for g in range(4):
            message = jnp.where(lane == g * 4 + s, total[g * 8 : (g + 1) * 8, :], message)
        message = jnp.where(lane == 16 + s, places[2, s].astype(F32), message)
    mine[...] = message

    def copy(src, dst, sem, k, device):
        return pltpu.make_async_remote_copy(
            src_ref=src, dst_ref=dst, send_sem=send_sem.at[k], recv_sem=sem,
            device_id=(device,), device_id_type=MESH,
        )

    @pl.when(core == 1)
    def _():
        pl.semaphore_wait(barrier, 1)
        up = copy(mine, half, half_sem, 0, me - 1)
        up.start()
        up.wait_send()
        copy(send, result, back_sem, 0, me - 1).wait_recv()
        out_ref[...] = result[...]

    @pl.when(even)
    def _():
        pl.semaphore_wait(barrier, 19)
        copy(mine, half, half_sem, 0, me + 1).wait_recv()
        both = mine[...] + half[...]
        across[0] = both
        rows = [copy(across.at[0], across.at[k], across_sem.at[k], k, other_x(k)) for k in range(1, 4)]
        for c in rows:
            c.start()
        group = both
        before = jnp.zeros((8, W), F32)
        for k in range(1, 4):
            rows[k - 1].wait_recv()
            piece = across[k]
            group = group + piece
            before = before + jnp.where((x + 4 - k) % 4 < x, piece, 0.0)
        plane[0] = group
        far = [copy(plane.at[0], plane.at[k], plane_sem.at[k], 3 + k, other_plane(k)) for k in range(1, 16)]
        for c in far:
            c.start()
        for k in range(1, 16):
            far[k - 1].wait_recv()
            before = before + jnp.where((zy + 16 - k) % 16 < zy, plane[k], 0.0)
        out_ref[...] = before
        send[...] = before + mine[...]
        back = copy(send, result, back_sem, 0, me + 1)
        back.start()
        for c in rows + far:
            c.wait_send()
        back.wait_send()


def scan(places, totals):
    tile = pltpu.VMEM((8, W), F32)
    return pl.pallas_call(
        scan_kernel,
        in_specs=[SMEM] + [VMEM] * 4,
        out_specs=VMEM,
        out_shape=shape(8, W),
        scratch_shapes=[
            tile, tile, pltpu.VMEM((4, 8, W), F32), pltpu.VMEM((16, 8, W), F32), tile, tile,
            pltpu.SemaphoreType.DMA, pltpu.SemaphoreType.DMA((4,)), pltpu.SemaphoreType.DMA((16,)),
            pltpu.SemaphoreType.DMA, pltpu.SemaphoreType.DMA((19,)),
        ],
        compiler_params=pltpu.CompilerParams(collective_id=0, has_side_effects=True),
        cost_estimate=pl.CostEstimate(flops=8_000_000_000, bytes_accessed=2**20, transcendentals=0),
        name="scan",
    )(places, *totals)


def finish_kernel(s, chunk, at, before_ref, rank_ref, prefix_ref, tail_hbm, early_hbm, *rest):
    mean_ref, deviation_ref, table, sems = rest[-4:]

    @pl.when(pl.program_id(0) == 0)
    def _():
        a = pltpu.make_async_copy(tail_hbm, table.at[:, pl.ds(0, SPAN)], sems.at[0])
        b = pltpu.make_async_copy(early_hbm, table.at[:, pl.ds(SPAN, EARLY)], sems.at[1])
        a.start()
        b.start()
        a.wait()
        b.wait()

    before = jnp.concatenate([before_ref[:, g * 4 + s : g * 4 + s + 1] for g in range(4)], axis=0)
    before = jnp.broadcast_to(before, (COLS, W))
    seen = jnp.broadcast_to(before_ref[0:1, 16 + s : 17 + s], (1, W))
    group = 4

    def body(g, _):
        for u in range(group):
            k = g * group + u
            t = pl.program_id(0) * (chunk // W) + k
            row = STREAMS * t + s
            lanes = pl.ds(pl.multiple_of(k * W, W), W)
            rank = rank_ref[pl.ds(row, 1), :]
            block = at[0, row] // W
            where = rank - block * W
            index = jnp.broadcast_to(where & (W - 1), (COLS, W))
            near = table[:, pl.ds(pl.multiple_of(block * W, W), W)]
            next_ = table[:, pl.ds(pl.multiple_of(block * W + W, W), W)]
            earlier = jnp.where(where >= W, lane_gather(next_, index), lane_gather(near, index))
            prefix = prefix_ref[:, lanes]
            mean = (prefix - earlier) * (1.0 / SPAN)
            inverse = 1.0 / jnp.maximum(seen + rank.astype(F32), 1.0)
            mean_ref[0, :, lanes] = mean
            deviation_ref[0, :, lanes] = mean - (before + prefix) * inverse
        return 0

    lax.fori_loop(0, chunk // W // group, body, 0)


def finish(s, places, before, rank, prefix, tail, early, partial_outs):
    chunk = 2048
    n = TILES * STREAMS
    block = pl.BlockSpec((1, COLS, chunk), lambda i: (s, 0, i))
    whole_out = shape(STREAMS, COLS, ROWS)
    return pl.pallas_call(
        functools.partial(finish_kernel, s, chunk),
        grid=(ROWS // chunk,),
        in_specs=[
            SMEM, whole(8, W), whole(n, W), pl.BlockSpec((COLS, chunk), lambda i: (0, i)), HBM, HBM,
        ] + [HBM] * len(partial_outs),
        out_specs=[block, block],
        out_shape=[whole_out, whole_out],
        scratch_shapes=[pltpu.VMEM((COLS, TABLE + W), F32), pltpu.SemaphoreType.DMA((2,))],
        input_output_aliases={6: 0, 7: 1} if partial_outs else {},
        compiler_params=PARAMS,
        cost_estimate=COST,
        name=f"finish_{s}",
    )(places, before, rank, prefix, tail, early, *partial_outs)


def per_device(events, keep):
    count = lax.axis_size("rows")
    chain = [(d, d + 1) for d in range(count - 1)]
    keepf, src, rank, places, *first = pack_first(events, keep)
    packed = [first]
    tails = [lax.ppermute(first[1], "rows", chain)]
    for s in range(1, STREAMS):
        packed.append(pack_stream(s, places, events, keepf, src))
        tails.append(lax.ppermute(packed[s][1], "rows", chain))
    before = scan(places, [p[3] for p in packed])
    outs = ()
    for s in range(STREAMS):
        prefix, _, early, _ = packed[s]
        outs = finish(s, places, before, rank, prefix, tails[s], early, outs)
    return tuple(outs)


def solution(mesh):
    in_specs = (P(None, None, "rows"), P(None, "rows"))
    out_specs = (P(None, None, "rows"), P(None, None, "rows"))
    return jax.shard_map(per_device, mesh=mesh, in_specs=in_specs, out_specs=out_specs, check_vma=False)
```

```python
import jax
import jax.numpy as jnp
from jax import lax
from jax.experimental import pallas as pl
from jax.experimental.pallas import tpu as pltpu
from jax.sharding import PartitionSpec as P

SPAN = 4096
W = 128
STREAMS = 4
COLS = 32
ROWS = 8192
TILES = ROWS // W
LEAD = 8
TABLE = TILES + LEAD + 2
EARLY = SPAN + W
N = TILES * STREAMS
MESH = pl.DeviceIdType.MESH
F32 = jnp.float32
I32 = jnp.int32
BF16 = jnp.bfloat16


def lanes_of(shape):
    return lax.broadcasted_iota(I32, shape, len(shape) - 1)


def rows_of(shape):
    return lax.broadcasted_iota(I32, shape, 0)


def lane_gather(values, index):
    return jnp.take_along_axis(values, index, axis=1, mode="promise_in_bounds")


def dot(a, b):
    return jnp.dot(a, b, preferred_element_type=F32)


def make_weights(w_ref):
    r = rows_of(w_ref.shape) % W
    c = lanes_of(w_ref.shape)
    w_ref[...] = ((r <= c % W) | (c >= W)).astype(F32).astype(BF16)


def index_maps(keep_ref, keepi_ref, keepf_ref, src_ref, rank_ref, places_ref, moves_ref):
    for t in range(TILES):
        keepi_ref[pl.ds(STREAMS * t, STREAMS), :] = keep_ref[:, t * W : (t + 1) * W]
    keep = keepi_ref[...].astype(F32)
    keepf_ref[...] = keep
    keep = keep.astype(BF16)
    tri = (rows_of((W, W)) <= lanes_of((W, W))).astype(F32).astype(BF16)
    ones = jnp.ones((W, W), BF16)
    inside = dot(keep, tri)
    count = dot(keep, ones)
    counts = count.astype(BF16)
    ri, ci = rows_of((N, N)), lanes_of((N, N))
    same = (ri & (STREAMS - 1)) == (ci & (STREAMS - 1))
    before = (same & ((ci >> 2) < (ri >> 2))).astype(F32).astype(BF16)
    same = same.astype(F32).astype(BF16)
    count_row = jnp.sum(keepi_ref[...].T, axis=0, keepdims=True)
    count_row = jnp.broadcast_to(count_row, (8, N))
    start_row = count_row
    for k in range(6):
        step = STREAMS << k
        start_row = start_row + jnp.where(lanes_of((8, N)) >= step, pltpu.roll(start_row, step, 1), 0)
    places_ref[...] = jnp.where(rows_of((8, N)) == 0, start_row - count_row, start_row)
    start = dot(before, counts).astype(I32)
    total = dot(same, counts).astype(I32)
    inside = inside.astype(I32)
    rank_ref[...] = start + inside
    place = start - total + ROWS
    wanted = (lanes_of((N, W)) - place) & (W - 1)
    way = jnp.where(wanted < count.astype(I32), ((place + wanted) >> 7) - (rows_of((N, W)) >> 2), 0)
    for k in range(6):
        step = STREAMS << k
        moves = (way >> k) & 1
        moves_ref[k, STREAMS * LEAD :, :] = moves
        moves_ref[k, : STREAMS * LEAD, :] = jnp.zeros((STREAMS * LEAD, W), I32)
        arrives = pltpu.roll(moves, step, 0)
        way = jnp.where(arrives == 1, pltpu.roll(way, step, 0), jnp.where(moves == 1, 0, way))
    found = jnp.zeros((N, W), I32)
    for step in (64, 32, 16, 8, 4, 2, 1):
        probe = lane_gather(inside, found + (step - 1))
        found = jnp.where(probe <= wanted, found + step, found)
    src_ref[...] = found
    return total[0:8, :].astype(F32)


def prefixes(s, events_ref, keepf_ref, w_ref, prefix_ref, exclusive):
    group = 16

    def body(g, base):
        kept, lhs = [], []
        for u in range(group):
            t = g * group + u
            x = events_ref[:, pl.ds(pl.multiple_of(t * W, W), W)]
            x = x * keepf_ref[pl.ds(STREAMS * t + s, 1), :]
            kept.append(x)
            hi = x.astype(BF16)
            lhs.append(jnp.concatenate([hi, (x - hi.astype(F32)).astype(BF16)], axis=1))
        sums = dot(jnp.concatenate(lhs, axis=0), w_ref[...])
        for u in range(group):
            part = sums[u * COLS : (u + 1) * COLS]
            prefix = base + part[:, :W]
            base = base + part[:, W:]
            prefix_ref[g * group + u] = prefix
            exclusive[g * group + u] = prefix - kept[u]
        return base

    return lax.fori_loop(0, TILES // group, body, jnp.zeros((COLS, W), F32))


def tile_at(t):
    return pl.ds(pl.multiple_of(t * W, W), W)


def compact(s, src_ref, moves_ref, exclusive, table):
    group = 16

    def gather(g, _):
        for u in range(group):
            t = g * group + u
            index = jnp.broadcast_to(src_ref[pl.ds(STREAMS * t + s, 1), :], (COLS, W))
            table[t + LEAD] = lane_gather(exclusive[t], index)
        return 0

    lax.fori_loop(0, TILES // group, gather, 0)
    for k in range(6):
        step = 1 << k
        blocks = (TILES - step) // LEAD if step >= LEAD else TILES // LEAD

        def shift(g, _):
            moved = []
            for u in range(LEAD):
                t = TILES - 1 - g * LEAD - u
                moves = moves_ref[k, pl.ds(STREAMS * (t - step + LEAD) + s, 1), :]
                moved.append(
                    jnp.where(moves == 1, table[t - step + LEAD], table[t + LEAD])
                )
            for u in range(LEAD):
                table[TILES - 1 - g * LEAD - u + LEAD] = moved[u]
            return 0

        lax.fori_loop(0, blocks, shift, 0)


def take_tail(table, total, tail_ref):
    for t in range(SPAN // W):
        tail_ref[t] = table[LEAD + SPAN // W + t] - total


def take_early(s, at, table, windows):
    lane = lanes_of((COLS, W))
    first = ROWS - at[1, N - STREAMS + s]
    block, shift = jnp.minimum(first >> 7, SPAN // W), first & (W - 1)
    turn = (lane + shift) & (W - 1)
    fresh = lane < W - shift

    def rolled(j):
        return lane_gather(table[block + j + LEAD], turn)

    def early(g, now):
        for u in range(11):
            j = g * 11 + u
            following = rolled(j + 1)
            windows[SPAN // W + j] = jnp.where(fresh, now, following)
            now = following
        return now

    lax.fori_loop(0, EARLY // W // 11, early, rolled(0))


def finish(s, at, notes, rank_ref, prefix_ref, windows, mean_ref, deviation_ref):
    before = jnp.concatenate([notes[:, g * 4 + s : g * 4 + s + 1] for g in range(4)], axis=0)
    before = jnp.broadcast_to(before, (COLS, W))
    seen = jnp.broadcast_to(notes[0:1, 16 + s : 17 + s], (1, W))
    group = 16

    def body(g, _):
        for u in range(group):
            t = g * group + u
            row = STREAMS * t + s
            rank = rank_ref[pl.ds(row, 1), :]
            block = at[0, row] >> 7
            where = rank - (block << 7)
            index = jnp.broadcast_to(where & (W - 1), (COLS, W))
            near = windows[block]
            next_ = windows[block + 1]
            earlier = jnp.where(where >= W, lane_gather(next_, index), lane_gather(near, index))
            prefix = prefix_ref[t]
            mean = (prefix - earlier) * (1.0 / SPAN)
            inverse = 1.0 / jnp.maximum(seen + rank.astype(F32), 1.0)
            mean_ref[:, tile_at(t)] = mean
            deviation_ref[:, tile_at(t)] = mean - (before + prefix) * inverse
        return 0

    lax.fori_loop(0, TILES // group, body, 0)


def kernel(
    keep_hbm, events_hbm,
    mean_ref, deviation_ref,
    keep_ref, events, w_ref, keepi_ref, keepf_ref, src_ref, rank_ref, places_ref, moves_ref, at,
    prefix_ref, exclusive, table, tail, windows0, windows1, windows2, windows3,
    mine, half, across, plane, send, result,
    local_sem, tail_send, tail_recv, half_sem, across_sem, plane_sem, back_sem, scan_send,
):
    windows = (windows0, windows1, windows2, windows3)
    loads = [pltpu.make_async_copy(keep_hbm, keep_ref, local_sem.at[0])]
    for s in range(STREAMS):
        loads.append(pltpu.make_async_copy(events_hbm.at[s], events.at[s], local_sem.at[1 + s]))
    for load in loads:
        load.start()
    devices = lax.axis_size("rows")
    me = lax.axis_index("rows")
    core, chip = me % 2, me // 2
    x, zy = chip % 4, chip // 4
    even = core == 0

    def other_x(step):
        return (zy * 4 + (x + step) % 4) * 2

    def other_plane(step):
        return (((zy + step) % 16) * 4 + x) * 2

    barrier = pltpu.get_barrier_semaphore()

    def greet(device):
        pl.semaphore_signal(barrier, inc=1, device_id=(device,), device_id_type=MESH)

    def remote(src, dst, send_sem, recv_sem, device):
        return pltpu.make_async_remote_copy(
            src_ref=src, dst_ref=dst, send_sem=send_sem, recv_sem=recv_sem,
            device_id=(device,), device_id_type=MESH,
        )

    following = jnp.minimum(me + 1, devices - 1)

    @pl.when(me > 0)
    def _():
        greet(me - 1)

    @pl.when(me < devices - 1)
    def _():
        greet(me + 1)

    @pl.when(even)
    def _():
        for step in range(1, 4):
            greet(other_x(step))
        for step in range(1, 16):
            greet(other_plane(step))

    make_weights(w_ref)
    loads[0].wait()
    totals = index_maps(keep_ref, keepi_ref, keepf_ref, src_ref, rank_ref, places_ref, moves_ref)
    places = pltpu.make_async_copy(places_ref, at, local_sem.at[5])
    places.start()

    @pl.when(me == 0)
    def _():
        pl.semaphore_wait(barrier, 19)

    @pl.when((me > 0) & even)
    def _():
        pl.semaphore_wait(barrier, 20)

    @pl.when((core == 1) & (me < devices - 1))
    def _():
        pl.semaphore_wait(barrier, 2)

    @pl.when(me == devices - 1)
    def _():
        pl.semaphore_wait(barrier, 1)

    def tail_copy(s):
        return remote(
            tail.at[s], windows[s].at[pl.ds(0, SPAN // W)], tail_send.at[s], tail_recv.at[s], following
        )

    lane = lanes_of((8, W))
    message = jnp.zeros((8, W), F32)
    for s in range(STREAMS):
        loads[1 + s].wait()
        total = prefixes(s, events.at[s], keepf_ref, w_ref, prefix_ref.at[s], exclusive)
        compact(s, src_ref, moves_ref, exclusive, table)
        take_tail(table, total, tail.at[s])

        @pl.when(me < devices - 1)
        def _():
            tail_copy(s).start()

        if s == 0:
            places.wait()
        take_early(s, at, table, windows[s])
        for g in range(4):
            message = jnp.where(lane == g * 4 + s, total[g * 8 : (g + 1) * 8, :], message)
        message = jnp.where(lane == 16 + s, totals[s : s + 1, :], message)
    mine[...] = message

    @pl.when(core == 1)
    def _():
        up = remote(mine, half, scan_send.at[0], half_sem, me - 1)
        up.start()
        up.wait_send()
        remote(send, result, scan_send.at[0], back_sem, me - 1).wait_recv()

    @pl.when(even)
    def _():
        remote(mine, half, scan_send.at[0], half_sem, me + 1).wait_recv()
        both = mine[...] + half[...]
        across[0] = both
        rows = [
            remote(across.at[0], across.at[k], scan_send.at[k], across_sem.at[k], other_x(k))
            for k in range(1, 4)
        ]
        for c in rows:
            c.start()
        group = both
        before = jnp.zeros((8, W), F32)
        for k in range(1, 4):
            rows[k - 1].wait_recv()
            piece = across[k]
            group = group + piece
            before = before + jnp.where((x + 4 - k) % 4 < x, piece, 0.0)
        plane[0] = group
        far = [
            remote(plane.at[0], plane.at[k], scan_send.at[3 + k], plane_sem.at[k], other_plane(k))
            for k in range(1, 16)
        ]
        for c in far:
            c.start()
        for k in range(1, 16):
            far[k - 1].wait_recv()
            before = before + jnp.where((zy + 16 - k) % 16 < zy, plane[k], 0.0)
        result[...] = before
        send[...] = before + mine[...]
        back = remote(send, result, scan_send.at[0], back_sem, me + 1)
        back.start()
        for c in rows + far:
            c.wait_send()
        back.wait_send()

    notes = result[...]

    @pl.when(me == 0)
    def _():
        for s in range(STREAMS):
            for t in range(SPAN // W):
                windows[s][t] = jnp.zeros((COLS, W), F32)

    for s in range(STREAMS):

        @pl.when(me > 0)
        def _():
            tail_copy(s).wait_recv()

        finish(s, at, notes, rank_ref, prefix_ref.at[s], windows[s], mean_ref.at[s], deviation_ref.at[s])

    @pl.when(me < devices - 1)
    def _():
        for s in range(STREAMS):
            tail_copy(s).wait_send()


def per_device(events, keep):
    out = jax.ShapeDtypeStruct((STREAMS, COLS, ROWS), F32)
    tile = pltpu.VMEM((8, W), F32)
    dma = pltpu.SemaphoreType.DMA
    hbm = pl.BlockSpec(memory_space=pltpu.HBM)
    vmem = pl.BlockSpec(memory_space=pltpu.VMEM)
    return pl.pallas_call(
        kernel,
        in_specs=[hbm, hbm],
        out_specs=[vmem, vmem],
        out_shape=[out, out],
        scratch_shapes=[
            pltpu.VMEM((STREAMS, ROWS), I32),
            pltpu.VMEM((STREAMS, COLS, ROWS), F32),
            pltpu.VMEM((2 * W, 2 * W), BF16),
            pltpu.VMEM((N, W), I32),
            pltpu.VMEM((N, W), F32),
            pltpu.VMEM((N, W), I32),
            pltpu.VMEM((N, W), I32),
            pltpu.VMEM((8, N), I32),
            pltpu.VMEM((6, N + STREAMS * LEAD, W), I32),
            pltpu.SMEM((8, N), I32),
            pltpu.VMEM((STREAMS, TILES, COLS, W), F32),
            pltpu.VMEM((TILES, COLS, W), F32),
            pltpu.VMEM((TABLE, COLS, W), F32),
            pltpu.VMEM((STREAMS, SPAN // W, COLS, W), F32),
        ]
        + [pltpu.VMEM((TILES + 3, COLS, W), F32)] * STREAMS
        + [
            tile, tile, pltpu.VMEM((4, 8, W), F32), pltpu.VMEM((16, 8, W), F32), tile, tile,
            dma((6,)), dma((STREAMS,)), dma((STREAMS,)), dma, dma((4,)), dma((16,)), dma, dma((19,)),
        ],
        compiler_params=pltpu.CompilerParams(
            collective_id=0, has_side_effects=True, vmem_limit_bytes=44 * 2**20
        ),
        name="windows",
    )(keep, events)


def solution(mesh):
    in_specs = (P(None, None, "rows"), P(None, "rows"))
    out_specs = (P(None, None, "rows"), P(None, None, "rows"))
    return jax.shard_map(per_device, mesh=mesh, in_specs=in_specs, out_specs=out_specs, check_vma=False)
```

```python
import jax
import jax.numpy as jnp
from jax import lax
from jax.experimental import pallas as pl
from jax.experimental.pallas import tpu as pltpu
from jax.sharding import PartitionSpec as P

SPAN = 4096
W = 128
STREAMS = 4
COLS = 32
ROWS = 8192
TILES = ROWS // W
LEAD = 8
TABLE = TILES + LEAD + 2
EARLY = SPAN + W
N = TILES * STREAMS
UNITS = ((0, 3), (0, 2), (1, 3), (1, 2))
BACK = [[g for t, g in UNITS if t == s] for s in range(STREAMS)]
RELAYS_MIDDLE = ((), (), ((1, 1),), ((2, 1), (1, 2)))
RELAYS = ((), ((0, 1),), ((0, 2),), ((3, 1), (2, 2), (3, 2)))
ORDER = (2, 0, 1, 3)
MESH = pl.DeviceIdType.MESH
F32 = jnp.float32
I32 = jnp.int32
BF16 = jnp.bfloat16


def lanes_of(shape):
    return lax.broadcasted_iota(I32, shape, len(shape) - 1)


def rows_of(shape):
    return lax.broadcasted_iota(I32, shape, 0)


def lane_gather(values, index):
    return jnp.take_along_axis(values, index, axis=1, mode="promise_in_bounds")


def dot(a, b):
    return jnp.dot(a, b, preferred_element_type=F32)


def make_weights(w_ref):
    r = rows_of(w_ref.shape) % W
    c = lanes_of(w_ref.shape)
    w_ref[...] = ((r <= c % W) | (c >= W)).astype(F32).astype(BF16)


def index_maps(keep_ref, keepi_ref, keepf_ref, src_ref, rank_ref, places_ref, moves_ref):
    for t in range(TILES):
        keepi_ref[pl.ds(STREAMS * t, STREAMS), :] = keep_ref[:, t * W : (t + 1) * W]
    keep = keepi_ref[...].astype(F32)
    keepf_ref[...] = keep
    keep = keep.astype(BF16)
    tri = (rows_of((W, W)) <= lanes_of((W, W))).astype(F32).astype(BF16)
    ones = jnp.ones((W, W), BF16)
    inside = dot(keep, tri)
    count = dot(keep, ones)
    counts = count.astype(BF16)
    ri, ci = rows_of((N, N)), lanes_of((N, N))
    same = (ri & (STREAMS - 1)) == (ci & (STREAMS - 1))
    before = (same & ((ci >> 2) < (ri >> 2))).astype(F32).astype(BF16)
    same = same.astype(F32).astype(BF16)
    turned = keepi_ref[...].T
    count_row = jnp.sum(turned, axis=0, keepdims=True)
    count_row = jnp.broadcast_to(count_row, (8, N))
    start_row = count_row
    for k in range(6):
        step = STREAMS << k
        start_row = start_row + jnp.where(lanes_of((8, N)) >= step, pltpu.roll(start_row, step, 1), 0)
    start_row = start_row - count_row
    sub = rows_of((8, N))
    first_row = jnp.broadcast_to(turned[0:1], (8, N))
    places_ref[...] = start_row + jnp.where(sub == 1, count_row, jnp.where(sub == 2, first_row, 0))
    start = dot(before, counts).astype(I32)
    total = dot(same, counts).astype(I32)
    inside = inside.astype(I32)
    rank_ref[...] = start + inside
    place = start - total + ROWS
    wanted = (lanes_of((N, W)) - place) & (W - 1)
    way = jnp.where(wanted < count.astype(I32), ((place + wanted) >> 7) - (rows_of((N, W)) >> 2), 0)
    for k in range(6):
        step = STREAMS << k
        moves = (way >> k) & 1
        moves_ref[k, STREAMS * LEAD :, :] = moves
        moves_ref[k, : STREAMS * LEAD, :] = jnp.zeros((STREAMS * LEAD, W), I32)
        arrives = pltpu.roll(moves, step, 0)
        way = jnp.where(arrives == 1, pltpu.roll(way, step, 0), jnp.where(moves == 1, 0, way))
    found = jnp.zeros((N, W), I32)
    for step in (64, 32, 16, 8, 4, 2, 1):
        probe = lane_gather(inside, found + (step - 1))
        found = jnp.where(probe <= wanted, found + step, found)
    src_ref[...] = found
    return total[0:8, :].astype(F32)


def prefixes(s, events_ref, keepf_ref, w_ref, prefix_ref, exclusive):
    group = 16

    def body(g, base):
        kept, lhs = [], []
        for u in range(group):
            t = g * group + u
            x = events_ref[:, pl.ds(pl.multiple_of(t * W, W), W)]
            x = x * keepf_ref[pl.ds(STREAMS * t + s, 1), :]
            kept.append(x)
            hi = x.astype(BF16)
            lhs.append(jnp.concatenate([hi, (x - hi.astype(F32)).astype(BF16)], axis=1))
        sums = dot(jnp.concatenate(lhs, axis=0), w_ref[...])
        for u in range(group):
            part = sums[u * COLS : (u + 1) * COLS]
            prefix = base + part[:, :W]
            base = base + part[:, W:]
            prefix_ref[g * group + u] = prefix
            exclusive[g * group + u] = prefix - kept[u]
        return base

    return lax.fori_loop(0, TILES // group, body, jnp.zeros((COLS, W), F32))


def tile_at(t):
    return pl.ds(pl.multiple_of(t * W, W), W)


def compact(s, src_ref, moves_ref, exclusive, table):
    group = 16

    def gather(g, _):
        for u in range(group):
            t = g * group + u
            index = jnp.broadcast_to(src_ref[pl.ds(STREAMS * t + s, 1), :], (COLS, W))
            table[t + LEAD] = lane_gather(exclusive[t], index)
        return 0

    lax.fori_loop(0, TILES // group, gather, 0)
    for k in range(6):
        step = 1 << k
        blocks = (TILES - step) // LEAD if step >= LEAD else TILES // LEAD

        def shift(g, _):
            moved = []
            for u in range(LEAD):
                t = TILES - 1 - g * LEAD - u
                moves = moves_ref[k, pl.ds(STREAMS * (t - step + LEAD) + s, 1), :]
                moved.append(
                    jnp.where(moves == 1, table[t - step + LEAD], table[t + LEAD])
                )
            for u in range(LEAD):
                table[TILES - 1 - g * LEAD - u + LEAD] = moved[u]
            return 0

        lax.fori_loop(0, blocks, shift, 0)


def take_tail(table, total, tail_ref):
    for t in range(SPAN // W):
        tail_ref[t] = table[LEAD + SPAN // W + t] - total


def take_early(s, at, table, windows):
    lane = lanes_of((COLS, W))
    first = ROWS - at[1, N - STREAMS + s]
    block, shift = jnp.minimum(first >> 7, SPAN // W), first & (W - 1)
    turn = (lane + shift) & (W - 1)
    fresh = lane < W - shift

    def rolled(j):
        return lane_gather(table[block + j + LEAD], turn)

    def early(g, now):
        for u in range(11):
            j = g * 11 + u
            following = rolled(j + 1)
            windows[SPAN // W + j] = jnp.where(fresh, now, following)
            now = following
        return now

    lax.fori_loop(0, EARLY // W // 11, early, rolled(0))


def finish(s, at, notes, rank_ref, prefix_ref, windows, mean_ref, deviation_ref):
    before = jnp.concatenate([notes[:, g * 4 + s : g * 4 + s + 1] for g in range(4)], axis=0)
    before = jnp.broadcast_to(before, (COLS, W))
    seen = jnp.broadcast_to(notes[0:1, 16 + s : 17 + s], (1, W))
    lane = lanes_of((COLS, W))
    group = 16

    def body(g, _):
        for u in range(group):
            t = g * group + u
            row = STREAMS * t + s
            rank = rank_ref[pl.ds(row, 1), :]
            block = at[0, row] >> 7
            index = jnp.broadcast_to(rank & (W - 1), (COLS, W))
            slots = jnp.where(lane >= at[2, row] - (block << 7), windows[block], windows[block + 1])
            earlier = lane_gather(slots, index)
            prefix = prefix_ref[t]
            mean = (prefix - earlier) * (1.0 / SPAN)
            inverse = 1.0 / jnp.maximum(seen + rank.astype(F32), 1.0)
            mean_ref[:, tile_at(t)] = mean
            deviation_ref[:, tile_at(t)] = mean - (before + prefix) * inverse
        return 0

    lax.fori_loop(0, TILES // group, body, 0)


def take_message(events, keepf_ref, totals):
    group = 4

    def body(g, sums):
        sums = list(sums)
        for u in range(group):
            t = g * group + u
            for s in range(STREAMS):
                sums[s] = sums[s] + events[s, :, tile_at(t)] * keepf_ref[pl.ds(STREAMS * t + s, 1), :]
        return tuple(sums)

    zero = jnp.zeros((COLS, W), F32)
    sums = lax.fori_loop(0, TILES // group, body, (zero,) * STREAMS)
    lane = lanes_of((8, W))
    message = jnp.zeros((8, W), F32)
    for s in range(STREAMS):
        total = jnp.sum(sums[s], axis=1, keepdims=True)
        for g in range(4):
            message = jnp.where(lane == g * 4 + s, total[g * 8 : (g + 1) * 8], message)
        message = jnp.where(lane == 16 + s, totals[s : s + 1, :], message)
    return message


def kernel(
    keep_ref, events_hbm,
    mean_ref, deviation_ref,
    events, w_ref, keepi_ref, keepf_ref, src_ref, rank_ref, places_ref, moves_ref, at,
    prefix_ref, exclusive, table, tail, windows0, windows1, windows2, windows3,
    relay, mine, half, across, plane, inside, given, send, result,
    local_sem, tail_send, tail_recv, half_sem, across_sem, plane_sem, given_sem, back_sem, scan_send,
    hop_send, hop_recv,
):
    windows = (windows0, windows1, windows2, windows3)
    loads = [None]
    for s in range(STREAMS):
        loads.append(pltpu.make_async_copy(events_hbm.at[s], events.at[s], local_sem.at[1 + s]))
    for load in loads[1:]:
        load.start()
    devices = lax.axis_size("rows")
    me = lax.axis_index("rows")
    core, chip = me % 2, me // 2
    x, zy = chip % 4, chip // 4
    even = core == 0

    def other_x(step):
        return (zy * 4 + (x + step) % 4) * 2

    def other_plane(step):
        return (((zy + step) % 16) * 4 + x) * 2

    barrier = pltpu.get_barrier_semaphore()

    def greet(device):
        pl.semaphore_signal(barrier, inc=1, device_id=(device,), device_id_type=MESH)

    def remote(src, dst, send_sem, recv_sem, device):
        return pltpu.make_async_remote_copy(
            src_ref=src, dst_ref=dst, send_sem=send_sem, recv_sem=recv_sem,
            device_id=(device,), device_id_type=MESH,
        )

    following, preceding = (me + 1) % devices, (me + devices - 1) % devices
    ahead, behind = (zy * 4 + (x + 1) % 4) * 2, (zy * 4 + (x + 3) % 4) * 2
    next_line, last_line = ((zy + 1) % 16 * 4 + 2) * 2 + 1, ((zy + 15) % 16 * 4 + 3) * 2 + 1
    first_relay = jnp.where(x == 3, next_line, behind + 1)
    starts = (core == 1) & (me < devices - 1)
    relays = (core == 1) & ((x != 2) | (zy > 0))
    relays_on = (core == 1) & ((x != 1) | (zy > 0))

    greet(following)
    greet(preceding)

    @pl.when(even)
    def _():
        for step in range(1, 4):
            greet(other_x(step))
        greet(ahead + 1)

    @pl.when(even & (x > 0))
    def _():
        for step in range(1, 16):
            greet(other_plane(step))

    @pl.when(core == 1)
    def _():
        greet(ahead + 1)
        greet(behind + 1)
        greet(behind)

    @pl.when((core == 1) & (x == 3))
    def _():
        greet(next_line)

    @pl.when((core == 1) & (x == 2))
    def _():
        greet(last_line)

    make_weights(w_ref)
    totals = index_maps(keep_ref, keepi_ref, keepf_ref, src_ref, rank_ref, places_ref, moves_ref)
    places = pltpu.make_async_copy(places_ref, at, local_sem.at[5])
    places.start()

    def everyone_is_here():
        @pl.when(even & (x == 0))
        def _():
            pl.semaphore_wait(barrier, 6)

        @pl.when(even & (x > 0))
        def _():
            pl.semaphore_wait(barrier, 21)

        @pl.when((core == 1) & (x < 2))
        def _():
            pl.semaphore_wait(barrier, 5)

        @pl.when((core == 1) & (x >= 2))
        def _():
            pl.semaphore_wait(barrier, 6)

    def whole_copy(s):
        return remote(
            tail.at[s], windows[s].at[pl.ds(0, SPAN // W)], tail_send.at[s], tail_recv.at[s], following
        )

    def part_copy(s):
        part = pl.ds(0, COLS - 8 * len(BACK[s]))
        return remote(
            tail.at[s, :, part], windows[s].at[pl.ds(0, SPAN // W), part],
            tail_send.at[s], tail_recv.at[s], following,
        )

    def hop(unit, k):
        s, group = UNITS[unit]
        part = pl.ds(8 * group, 8)
        src = tail.at[s, :, part] if k == 0 else relay.at[k - 1, unit]
        dst = windows[s].at[pl.ds(0, SPAN // W), part] if k == 2 else relay.at[k, unit]
        device = (first_relay, behind + 1, behind)[k]
        return remote(src, dst, hop_send.at[k, unit], hop_recv.at[k, unit], device)

    def pass_on(unit, k):
        @pl.when((relays, relays_on)[k - 1])
        def _():
            hop(unit, k - 1).wait_recv()
            hop(unit, k).start()

    def across_copy(k):
        return remote(across.at[0], across.at[k], scan_send.at[k], across_sem.at[k], other_x(k))

    def plane_copy(k):
        return remote(plane.at[0], plane.at[k], scan_send.at[3 + k], plane_sem.at[k], other_plane(k))

    up = remote(mine, half, scan_send.at[0], half_sem, preceding)
    back = remote(send, result, scan_send.at[0], back_sem, following)
    lines_copy = remote(given, result, scan_send.at[19], given_sem, behind)

    def scan_step(step):
        if step == 0:
            mine[...] = take_message(events, keepf_ref, totals)

            @pl.when(core == 1)
            def _():
                up.start()

        if step == 1:

            @pl.when(even)
            def _():
                up.wait_recv()
                across[0] = mine[...] + half[...]
                for k in range(1, 4):
                    across_copy(k).start()

        if step == 2:

            @pl.when(even & (x > 0))
            def _():
                group = across[0]
                before = jnp.zeros((8, W), F32)
                for k in range(1, 4):
                    across_copy(k).wait_recv()
                    piece = across[k]
                    group = group + piece
                    before = before + jnp.where((x + 4 - k) % 4 < x, piece, 0.0)
                inside[...] = before
                plane[0] = group
                for k in range(1, 16):
                    plane_copy(k).start()

        if step == 3:

            @pl.when(even & (x > 0))
            def _():
                lines = jnp.zeros((8, W), F32)
                for k in range(1, 16):
                    plane_copy(k).wait_recv()
                    lines = lines + jnp.where((zy + 16 - k) % 16 < zy, plane[k], 0.0)
                given[...] = lines
                result[...] = inside[...] + lines

            @pl.when(even & (x == 1))
            def _():
                lines_copy.start()

            @pl.when(even & (x == 0))
            def _():
                for k in range(1, 4):
                    across_copy(k).wait_recv()
                lines_copy.wait_recv()

            @pl.when(even)
            def _():
                send[...] = result[...] + mine[...]
                back.start()

            @pl.when(core == 1)
            def _():
                back.wait_recv()

    for s in range(STREAMS):
        if s == 0:
            loads[1].wait()
        total = prefixes(s, events.at[s], keepf_ref, w_ref, prefix_ref.at[s], exclusive)
        for unit, k in RELAYS_MIDDLE[s]:
            pass_on(unit, k)
        compact(s, src_ref, moves_ref, exclusive, table)
        take_tail(table, total, tail.at[s])
        if s == 0:
            everyone_is_here()

        @pl.when(even)
        def _():
            whole_copy(s).start()

        @pl.when(starts)
        def _():
            part_copy(s).start()
            for unit in range(len(UNITS)):
                if UNITS[unit][0] == s:
                    hop(unit, 0).start()

        if s == 0:
            for load in loads[2:]:
                load.wait()
            places.wait()
        for unit, k in RELAYS[s]:
            pass_on(unit, k)
        if s < 3:
            scan_step(s)
        take_early(s, at, table, windows[s])
    scan_step(3)

    notes = result[...]

    @pl.when(me == 0)
    def _():
        for s in range(STREAMS):
            for t in range(SPAN // W):
                windows[s][t] = jnp.zeros((COLS, W), F32)

    for s in ORDER:

        @pl.when(core == 1)
        def _():
            whole_copy(s).wait_recv()

        @pl.when(even & (me > 0))
        def _():
            part_copy(s).wait_recv()
            for unit in range(len(UNITS)):
                if UNITS[unit][0] == s:
                    hop(unit, 2).wait_recv()

        finish(s, at, notes, rank_ref, prefix_ref.at[s], windows[s], mean_ref.at[s], deviation_ref.at[s])

    @pl.when(even)
    def _():
        for s in range(STREAMS):
            whole_copy(s).wait_send()
        for k in range(1, 4):
            across_copy(k).wait_send()
        back.wait_send()

    @pl.when(core == 1)
    def _():
        up.wait_send()

    @pl.when(even & (x > 0))
    def _():
        for k in range(1, 16):
            plane_copy(k).wait_send()

    @pl.when(even & (x == 1))
    def _():
        lines_copy.wait_send()

    @pl.when(starts)
    def _():
        for s in range(STREAMS):
            part_copy(s).wait_send()
        for unit in range(len(UNITS)):
            hop(unit, 0).wait_send()

    for k, sender in ((1, relays), (2, relays_on)):

        @pl.when(sender)
        def _():
            for unit in range(len(UNITS)):
                hop(unit, k).wait_send()


def write_kernel(mean_ref, deviation_ref, mean_hbm, deviation_hbm, sems):
    copies = []
    for s in range(STREAMS):
        copies.append(pltpu.make_async_copy(mean_ref.at[s], mean_hbm.at[s], sems.at[2 * s]))
        copies.append(pltpu.make_async_copy(deviation_ref.at[s], deviation_hbm.at[s], sems.at[2 * s + 1]))
    for copy in copies:
        copy.start()
    for copy in copies:
        copy.wait()


def per_device(events, keep):
    out = jax.ShapeDtypeStruct((STREAMS, COLS, ROWS), F32)
    tile = pltpu.VMEM((8, W), F32)
    dma = pltpu.SemaphoreType.DMA
    hbm = pl.BlockSpec(memory_space=pltpu.HBM)
    vmem = pl.BlockSpec(memory_space=pltpu.VMEM)
    mean, deviation = pl.pallas_call(
        kernel,
        in_specs=[vmem, hbm],
        out_specs=[vmem, vmem],
        out_shape=[out, out],
        scratch_shapes=[
            pltpu.VMEM((STREAMS, COLS, ROWS), F32),
            pltpu.VMEM((2 * W, 2 * W), BF16),
            pltpu.VMEM((N, W), I32),
            pltpu.VMEM((N, W), F32),
            pltpu.VMEM((N, W), I32),
            pltpu.VMEM((N, W), I32),
            pltpu.VMEM((8, N), I32),
            pltpu.VMEM((6, N + STREAMS * LEAD, W), I32),
            pltpu.SMEM((8, N), I32),
            pltpu.VMEM((STREAMS, TILES, COLS, W), F32),
            pltpu.VMEM((TILES, COLS, W), F32),
            pltpu.VMEM((TABLE, COLS, W), F32),
            pltpu.VMEM((STREAMS, SPAN // W, COLS, W), F32),
        ]
        + [pltpu.VMEM((TILES + 3, COLS, W), F32)] * STREAMS
        + [
            pltpu.VMEM((2, len(UNITS), SPAN // W, 8, W), F32),
            tile, tile, pltpu.VMEM((4, 8, W), F32), pltpu.VMEM((16, 8, W), F32), tile, tile, tile, tile,
            dma((6,)), dma((STREAMS,)), dma((STREAMS,)), dma, dma((4,)), dma((16,)), dma, dma, dma((20,)),
            dma((3, len(UNITS))), dma((3, len(UNITS))),
        ],
        compiler_params=pltpu.CompilerParams(
            collective_id=0, has_side_effects=True, vmem_limit_bytes=44 * 2**20
        ),
        name="windows",
    )(keep, events)
    return pl.pallas_call(
        write_kernel,
        in_specs=[vmem, vmem],
        out_specs=[hbm, hbm],
        out_shape=[out, out],
        scratch_shapes=[dma((2 * STREAMS,))],
        compiler_params=pltpu.CompilerParams(vmem_limit_bytes=2**20),
        name="write",
    )(mean, deviation)


def solution(mesh):
    in_specs = (P(None, None, "rows"), P(None, "rows"))
    out_specs = (P(None, None, "rows"), P(None, None, "rows"))
    return jax.shard_map(per_device, mesh=mesh, in_specs=in_specs, out_specs=out_specs, check_vma=False)
```

```python
import jax
import jax.numpy as jnp
from jax import lax
from jax.experimental import pallas as pl
from jax.experimental.pallas import tpu as pltpu
from jax.sharding import PartitionSpec as P

SPAN = 4096
W = 128
STREAMS = 4
COLS = 32
ROWS = 8192
TILES = ROWS // W
LEAD = 8
TABLE = TILES + LEAD + 2
EARLY = SPAN + W
N = TILES * STREAMS
BASE = ((0, 3), (1, 3), (2, 3))
EXTRA = ((0, 2), (1, 2))
UNITS = BASE + EXTRA
RELAYS_MIDDLE = ((), (), ((0, 1), (3, 1)), ((1, 1), (4, 1)))
RELAYS_FIRST = ((), (), (), ((0, 2),))
RELAYS = ((), (), (), ((3, 2), (2, 1), (1, 2), (4, 2), (2, 2)))
ORDER = (0, 1, 2)
MESH = pl.DeviceIdType.MESH
F32 = jnp.float32
I32 = jnp.int32
BF16 = jnp.bfloat16


def lanes_of(shape):
    return lax.broadcasted_iota(I32, shape, len(shape) - 1)


def rows_of(shape):
    return lax.broadcasted_iota(I32, shape, 0)


def lane_gather(values, index):
    return jnp.take_along_axis(values, index, axis=1, mode="promise_in_bounds")


def dot(a, b):
    return jnp.dot(a, b, preferred_element_type=F32)


def make_weights(w_ref):
    r = rows_of(w_ref.shape) % W
    c = lanes_of(w_ref.shape)
    w_ref[...] = ((r <= c % W) | (c >= W)).astype(F32).astype(BF16)


def index_maps(keep_ref, keepi_ref, keepf_ref, src_ref, rank_ref, places_ref, moves_ref):
    for t in range(TILES):
        keepi_ref[pl.ds(STREAMS * t, STREAMS), :] = keep_ref[:, t * W : (t + 1) * W]
    keep = keepi_ref[...].astype(F32)
    keepf_ref[...] = keep
    keep = keep.astype(BF16)
    tri = (rows_of((W, W)) <= lanes_of((W, W))).astype(F32).astype(BF16)
    ones = jnp.ones((W, W), BF16)
    inside = dot(keep, tri)
    count = dot(keep, ones)
    counts = count.astype(BF16)
    ri, ci = rows_of((N, N)), lanes_of((N, N))
    same = (ri & (STREAMS - 1)) == (ci & (STREAMS - 1))
    before = (same & ((ci >> 2) < (ri >> 2))).astype(F32).astype(BF16)
    same = same.astype(F32).astype(BF16)
    turned = keepi_ref[...].T
    count_row = jnp.sum(turned, axis=0, keepdims=True)
    count_row = jnp.broadcast_to(count_row, (8, N))
    start_row = count_row
    for k in range(6):
        step = STREAMS << k
        start_row = start_row + jnp.where(lanes_of((8, N)) >= step, pltpu.roll(start_row, step, 1), 0)
    start_row = start_row - count_row
    sub = rows_of((8, N))
    first_row = jnp.broadcast_to(turned[0:1], (8, N))
    places_ref[...] = start_row + jnp.where(sub == 1, count_row, jnp.where(sub == 2, first_row, 0))
    start = dot(before, counts).astype(I32)
    total = dot(same, counts).astype(I32)
    inside = inside.astype(I32)
    rank_ref[...] = start + inside
    place = start - total + ROWS
    wanted = (lanes_of((N, W)) - place) & (W - 1)
    way = jnp.where(wanted < count.astype(I32), ((place + wanted) >> 7) - (rows_of((N, W)) >> 2), 0)
    for k in range(6):
        step = STREAMS << k
        moves = (way >> k) & 1
        moves_ref[k, STREAMS * LEAD :, :] = moves
        moves_ref[k, : STREAMS * LEAD, :] = jnp.zeros((STREAMS * LEAD, W), I32)
        arrives = pltpu.roll(moves, step, 0)
        way = jnp.where(arrives == 1, pltpu.roll(way, step, 0), jnp.where(moves == 1, 0, way))
    found = jnp.zeros((N, W), I32)
    for step in (64, 32, 16, 8, 4, 2, 1):
        probe = lane_gather(inside, found + (step - 1))
        found = jnp.where(probe <= wanted, found + step, found)
    src_ref[...] = found
    return total[0:8, :].astype(F32)


def prefixes(s, events_ref, keepf_ref, w_ref, prefix_ref, exclusive):
    group = 16

    def body(g, base):
        kept, lhs = [], []
        for u in range(group):
            t = g * group + u
            x = events_ref[:, pl.ds(pl.multiple_of(t * W, W), W)]
            x = x * keepf_ref[pl.ds(STREAMS * t + s, 1), :]
            kept.append(x)
            hi = x.astype(BF16)
            lhs.append(jnp.concatenate([hi, (x - hi.astype(F32)).astype(BF16)], axis=1))
        sums = dot(jnp.concatenate(lhs, axis=0), w_ref[...])
        for u in range(group):
            part = sums[u * COLS : (u + 1) * COLS]
            prefix = base + part[:, :W]
            base = base + part[:, W:]
            prefix_ref[g * group + u] = prefix
            exclusive[g * group + u] = prefix - kept[u]
        return base

    return lax.fori_loop(0, TILES // group, body, jnp.zeros((COLS, W), F32))


def tile_at(t):
    return pl.ds(pl.multiple_of(t * W, W), W)


def compact(s, src_ref, moves_ref, exclusive, table):
    group = 16

    def gather(g, _):
        for u in range(group):
            t = g * group + u
            index = jnp.broadcast_to(src_ref[pl.ds(STREAMS * t + s, 1), :], (COLS, W))
            table[t + LEAD] = lane_gather(exclusive[t], index)
        return 0

    lax.fori_loop(0, TILES // group, gather, 0)
    for k in range(6):
        step = 1 << k
        blocks = (TILES - step) // LEAD if step >= LEAD else TILES // LEAD

        def shift(g, _):
            moved = []
            for u in range(LEAD):
                t = TILES - 1 - g * LEAD - u
                moves = moves_ref[k, pl.ds(STREAMS * (t - step + LEAD) + s, 1), :]
                moved.append(
                    jnp.where(moves == 1, table[t - step + LEAD], table[t + LEAD])
                )
            for u in range(LEAD):
                table[TILES - 1 - g * LEAD - u + LEAD] = moved[u]
            return 0

        lax.fori_loop(0, blocks, shift, 0)


def take_tail(table, total, tail_ref):
    for t in range(SPAN // W):
        tail_ref[t] = table[LEAD + SPAN // W + t] - total


def take_early(s, at, table, windows):
    lane = lanes_of((COLS, W))
    first = ROWS - at[1, N - STREAMS + s]
    block, shift = jnp.minimum(first >> 7, SPAN // W), first & (W - 1)
    turn = (lane + shift) & (W - 1)
    fresh = lane < W - shift

    def rolled(j):
        return lane_gather(table[block + j + LEAD], turn)

    def early(g, now):
        for u in range(11):
            j = g * 11 + u
            following = rolled(j + 1)
            windows[SPAN // W + j] = jnp.where(fresh, now, following)
            now = following
        return now

    lax.fori_loop(0, EARLY // W // 11, early, rolled(0))


def finish(s, at, notes, rank_ref, prefix_ref, windows, mean_ref, deviation_ref):
    before = jnp.concatenate([notes[:, g * 4 + s : g * 4 + s + 1] for g in range(4)], axis=0)
    before = jnp.broadcast_to(before, (COLS, W))
    seen = jnp.broadcast_to(notes[0:1, 16 + s : 17 + s], (1, W))
    lane = lanes_of((COLS, W))
    group = 16

    def body(g, _):
        for u in range(group):
            t = g * group + u
            row = STREAMS * t + s
            rank = rank_ref[pl.ds(row, 1), :]
            block = at[0, row] >> 7
            index = jnp.broadcast_to(rank & (W - 1), (COLS, W))
            slots = jnp.where(lane >= at[2, row] - (block << 7), windows[block], windows[block + 1])
            earlier = lane_gather(slots, index)
            prefix = prefix_ref[t]
            mean = (prefix - earlier) * (1.0 / SPAN)
            inverse = 1.0 / jnp.maximum(seen + rank.astype(F32), 1.0)
            mean_ref[:, tile_at(t)] = mean
            deviation_ref[:, tile_at(t)] = mean - (before + prefix) * inverse
        return 0

    lax.fori_loop(0, TILES // group, body, 0)


def take_message(events, keepf_ref, totals):
    group = 4

    def body(g, sums):
        sums = list(sums)
        for u in range(group):
            t = g * group + u
            for s in range(STREAMS):
                sums[s] = sums[s] + events[s, :, tile_at(t)] * keepf_ref[pl.ds(STREAMS * t + s, 1), :]
        return tuple(sums)

    zero = jnp.zeros((COLS, W), F32)
    sums = lax.fori_loop(0, TILES // group, body, (zero,) * STREAMS)
    lane = lanes_of((8, W))
    message = jnp.zeros((8, W), F32)
    for s in range(STREAMS):
        total = jnp.sum(sums[s], axis=1, keepdims=True)
        for g in range(4):
            message = jnp.where(lane == g * 4 + s, total[g * 8 : (g + 1) * 8], message)
        message = jnp.where(lane == 16 + s, totals[s : s + 1, :], message)
    return message


def kernel(
    keep_ref, events_hbm,
    mean_ref, deviation_ref, rank_ref, places_ref, prefix3, windows3, notes_ref,
    events, w_ref, keepi_ref, keepf_ref, src_ref, moves_ref, at,
    prefix_ref, exclusive, tables, tail, windows0, windows1, windows2,
    relay, mine, half, across, plane, inside, given, send, result,
    local_sem, tail_send, tail_recv, half_sem, across_sem, plane_sem, given_sem, back_sem, scan_send,
    hop_send, hop_recv,
):
    windows = (windows0, windows1, windows2, windows3)
    prefix = [prefix_ref.at[s] for s in range(3)] + [prefix3]
    loads = [None]
    for s in range(STREAMS):
        loads.append(pltpu.make_async_copy(events_hbm.at[s], events.at[s], local_sem.at[1 + s]))
    for load in loads[1:]:
        load.start()
    devices = lax.axis_size("rows")
    me = lax.axis_index("rows")
    core, chip = me % 2, me // 2
    x, zy = chip % 4, chip // 4
    even = core == 0

    def other_x(step):
        return (zy * 4 + (x + step) % 4) * 2

    def other_plane(step):
        return (((zy + step) % 16) * 4 + x) * 2

    barrier = pltpu.get_barrier_semaphore()

    def greet(device):
        pl.semaphore_signal(barrier, inc=1, device_id=(device,), device_id_type=MESH)

    def remote(src, dst, send_sem, recv_sem, device):
        return pltpu.make_async_remote_copy(
            src_ref=src, dst_ref=dst, send_sem=send_sem, recv_sem=recv_sem,
            device_id=(device,), device_id_type=MESH,
        )

    following, preceding = (me + 1) % devices, (me + devices - 1) % devices
    ahead, behind = (zy * 4 + (x + 1) % 4) * 2, (zy * 4 + (x + 3) % 4) * 2
    next_line, last_line = ((zy + 1) % 16 * 4 + 2) * 2 + 1, ((zy + 15) % 16 * 4 + 3) * 2 + 1
    first_relay = jnp.where(x == 3, next_line, behind + 1)
    starts = (core == 1) & (me < devices - 1)
    relays = (core == 1) & ((x != 2) | (zy > 0))
    relays_on = (core == 1) & ((x != 1) | (zy > 0))

    greet(following)
    greet(preceding)

    @pl.when(even)
    def _():
        for step in range(1, 4):
            greet(other_x(step))
        greet(ahead + 1)

    @pl.when(even & (x > 0))
    def _():
        for step in range(1, 16):
            greet(other_plane(step))

    @pl.when(core == 1)
    def _():
        greet(ahead + 1)
        greet(behind + 1)
        greet(behind)

    @pl.when((core == 1) & (x == 3))
    def _():
        greet(next_line)

    @pl.when((core == 1) & (x == 2))
    def _():
        greet(last_line)

    make_weights(w_ref)
    totals = index_maps(keep_ref, keepi_ref, keepf_ref, src_ref, rank_ref, places_ref, moves_ref)
    places = pltpu.make_async_copy(places_ref, at, local_sem.at[5])
    places.start()

    def everyone_is_here():
        @pl.when(even & (x == 0))
        def _():
            pl.semaphore_wait(barrier, 6)

        @pl.when(even & (x > 0))
        def _():
            pl.semaphore_wait(barrier, 21)

        @pl.when((core == 1) & (x < 2))
        def _():
            pl.semaphore_wait(barrier, 5)

        @pl.when((core == 1) & (x >= 2))
        def _():
            pl.semaphore_wait(barrier, 6)

    def whole_copy(s):
        return remote(
            tail.at[s], windows[s].at[pl.ds(0, SPAN // W)], tail_send.at[s], tail_recv.at[s], following
        )

    def units_of(s, extra):
        return [u for u in range(len(UNITS)) if UNITS[u][0] == s and (extra or u < len(BASE))]

    def part_copy(s, extra):
        part = pl.ds(0, COLS - 8 * len(units_of(s, extra)))
        return remote(
            tail.at[s, :, part], windows[s].at[pl.ds(0, SPAN // W), part],
            tail_send.at[s], tail_recv.at[s], following,
        )

    def hop(unit, k):
        s, group = UNITS[unit]
        part = pl.ds(8 * group, 8)
        src = tail.at[s, :, part] if k == 0 else relay.at[k - 1, unit]
        dst = windows[s].at[pl.ds(0, SPAN // W), part] if k == 2 else relay.at[k, unit]
        device = (first_relay, behind + 1, behind)[k]
        return remote(src, dst, hop_send.at[k, unit], hop_recv.at[k, unit], device)

    def pass_on(unit, k):
        here = (relays, relays_on)[k - 1]
        if unit >= len(BASE):
            here = here & (x == 3 - k)

        @pl.when(here)
        def _():
            hop(unit, k - 1).wait_recv()
            hop(unit, k).start()

    def across_copy(k):
        return remote(across.at[0], across.at[k], scan_send.at[k], across_sem.at[k], other_x(k))

    def plane_copy(k):
        return remote(plane.at[0], plane.at[k], scan_send.at[3 + k], plane_sem.at[k], other_plane(k))

    up = remote(mine, half, scan_send.at[0], half_sem, preceding)
    back = remote(send, result, scan_send.at[0], back_sem, following)
    lines_copy = remote(given, result, scan_send.at[19], given_sem, behind)

    def scan_step(step):
        if step == 0:
            mine[...] = take_message(events, keepf_ref, totals)

            @pl.when(core == 1)
            def _():
                up.start()

        if step == 1:

            @pl.when(even)
            def _():
                up.wait_recv()
                across[0] = mine[...] + half[...]
                for k in range(1, 4):
                    across_copy(k).start()

        if step == 2:

            @pl.when(even & (x > 0))
            def _():
                group = across[0]
                before = jnp.zeros((8, W), F32)
                for k in range(1, 4):
                    across_copy(k).wait_recv()
                    piece = across[k]
                    group = group + piece
                    before = before + jnp.where((x + 4 - k) % 4 < x, piece, 0.0)
                inside[...] = before
                plane[0] = group
                for k in range(1, 16):
                    plane_copy(k).start()

        if step == 3:

            @pl.when(even & (x > 0))
            def _():
                lines = jnp.zeros((8, W), F32)
                for k in range(1, 16):
                    plane_copy(k).wait_recv()
                    lines = lines + jnp.where((zy + 16 - k) % 16 < zy, plane[k], 0.0)
                given[...] = lines
                result[...] = inside[...] + lines

            @pl.when(even & (x == 1))
            def _():
                lines_copy.start()

            @pl.when(even & (x > 0))
            def _():
                send[...] = result[...] + mine[...]
                back.start()

        if step == 4:

            @pl.when(even & (x == 0))
            def _():
                for k in range(1, 4):
                    across_copy(k).wait_recv()
                lines_copy.wait_recv()
                send[...] = result[...] + mine[...]
                back.start()

            @pl.when(core == 1)
            def _():
                back.wait_recv()

    for s in range(STREAMS):
        table = tables.at[s % 2]
        if s == 0:
            loads[1].wait()
        total = prefixes(s, events.at[s], keepf_ref, w_ref, prefix[s], exclusive)
        for unit, k in RELAYS_MIDDLE[s]:
            pass_on(unit, k)
        if s == 1:
            scan_step(1)
        if s == 3:
            scan_step(3)
        compact(s, src_ref, moves_ref, exclusive, table)
        take_tail(table, total, tail.at[s])
        if s == 0:
            everyone_is_here()
        for unit, k in RELAYS_FIRST[s]:
            pass_on(unit, k)

        @pl.when(even)
        def _():
            whole_copy(s).start()

        for extra in (False, True):

            @pl.when(starts & ((x == 3) == extra))
            def _():
                part_copy(s, extra).start()
                for unit in units_of(s, extra):
                    hop(unit, 0).start()

        if s == 0:
            for load in loads[2:]:
                load.wait()
            places.wait()
            scan_step(0)
        if s == 1:
            scan_step(2)
        if s > 0:
            take_early(s - 1, at, tables.at[(s - 1) % 2], windows[s - 1])
        for unit, k in RELAYS[s]:
            pass_on(unit, k)
    take_early(STREAMS - 1, at, tables.at[(STREAMS - 1) % 2], windows[STREAMS - 1])
    scan_step(4)
    notes = result[...]

    @pl.when(me == 0)
    def _():
        for s in range(STREAMS):
            for t in range(SPAN // W):
                windows[s][t] = jnp.zeros((COLS, W), F32)

    notes_ref[...] = notes

    def wait_tail(s):
        @pl.when(core == 1)
        def _():
            whole_copy(s).wait_recv()

        for extra in (False, True):

            @pl.when(even & (me > 0) & ((x == 0) == extra))
            def _():
                part_copy(s, extra).wait_recv()
                for unit in units_of(s, extra):
                    hop(unit, 2).wait_recv()

    for s in ORDER:
        wait_tail(s)
        finish(s, at, notes, rank_ref, prefix[s], windows[s], mean_ref.at[s], deviation_ref.at[s])
    wait_tail(3)

    @pl.when(even)
    def _():
        for s in range(STREAMS):
            whole_copy(s).wait_send()
        for k in range(1, 4):
            across_copy(k).wait_send()
        back.wait_send()

    @pl.when(core == 1)
    def _():
        up.wait_send()

    @pl.when(even & (x > 0))
    def _():
        for k in range(1, 16):
            plane_copy(k).wait_send()

    @pl.when(even & (x == 1))
    def _():
        lines_copy.wait_send()

    for extra in (False, True):

        @pl.when(starts & ((x == 3) == extra))
        def _():
            for s in range(STREAMS):
                part_copy(s, extra).wait_send()
                for unit in units_of(s, extra):
                    hop(unit, 0).wait_send()

    for k, sender in ((1, relays), (2, relays_on)):

        @pl.when(sender)
        def _():
            for unit in range(len(BASE)):
                hop(unit, k).wait_send()

        @pl.when(sender & (x == 3 - k))
        def _():
            for unit in range(len(BASE), len(UNITS)):
                hop(unit, k).wait_send()


def write_kernel(
    mean_ref, deviation_ref, rank_ref, places_ref, prefix_ref, windows, notes_ref,
    mean_hbm, deviation_hbm,
    mean, deviation, at, sems,
):
    places = pltpu.make_async_copy(places_ref, at, sems.at[0])
    places.start()
    copies = []
    for s in range(3):
        copies.append(pltpu.make_async_copy(mean_ref.at[s], mean_hbm.at[s], sems.at[2 * s + 1]))
        copies.append(pltpu.make_async_copy(deviation_ref.at[s], deviation_hbm.at[s], sems.at[2 * s + 2]))
    for copy in copies:
        copy.start()
    places.wait()
    finish(3, at, notes_ref[...], rank_ref, prefix_ref, windows, mean, deviation)
    copies.append(pltpu.make_async_copy(mean, mean_hbm.at[3], sems.at[7]))
    copies.append(pltpu.make_async_copy(deviation, deviation_hbm.at[3], sems.at[8]))
    for copy in copies[-2:]:
        copy.start()
    for copy in copies:
        copy.wait()


def per_device(events, keep):
    out = jax.ShapeDtypeStruct((STREAMS, COLS, ROWS), F32)
    tile = pltpu.VMEM((8, W), F32)
    dma = pltpu.SemaphoreType.DMA
    hbm = pl.BlockSpec(memory_space=pltpu.HBM)
    vmem = pl.BlockSpec(memory_space=pltpu.VMEM)
    three = jax.ShapeDtypeStruct((3, COLS, ROWS), F32)
    state = [
        three, three,
        jax.ShapeDtypeStruct((N, W), I32),
        jax.ShapeDtypeStruct((8, N), I32),
        jax.ShapeDtypeStruct((TILES, COLS, W), F32),
        jax.ShapeDtypeStruct((TILES + 3, COLS, W), F32),
        jax.ShapeDtypeStruct((8, W), F32),
    ]
    state = pl.pallas_call(
        kernel,
        in_specs=[vmem, hbm],
        out_specs=[vmem] * len(state),
        out_shape=state,
        scratch_shapes=[
            pltpu.VMEM((STREAMS, COLS, ROWS), F32),
            pltpu.VMEM((2 * W, 2 * W), BF16),
            pltpu.VMEM((N, W), I32),
            pltpu.VMEM((N, W), F32),
            pltpu.VMEM((N, W), I32),
            pltpu.VMEM((6, N + STREAMS * LEAD, W), I32),
            pltpu.SMEM((8, N), I32),
            pltpu.VMEM((3, TILES, COLS, W), F32),
            pltpu.VMEM((TILES, COLS, W), F32),
            pltpu.VMEM((2, TABLE, COLS, W), F32),
            pltpu.VMEM((STREAMS, SPAN // W, COLS, W), F32),
        ]
        + [pltpu.VMEM((TILES + 3, COLS, W), F32)] * 3
        + [
            pltpu.VMEM((2, len(UNITS), SPAN // W, 8, W), F32),
            tile, tile, pltpu.VMEM((4, 8, W), F32), pltpu.VMEM((16, 8, W), F32), tile, tile, tile, tile,
            dma((6,)), dma((STREAMS,)), dma((STREAMS,)), dma, dma((4,)), dma((16,)), dma, dma, dma((20,)),
            dma((3, len(UNITS))), dma((3, len(UNITS))),
        ],
        compiler_params=pltpu.CompilerParams(
            collective_id=0, has_side_effects=True, vmem_limit_bytes=43 * 2**20
        ),
        name="windows",
    )(keep, events)
    return pl.pallas_call(
        write_kernel,
        in_specs=[vmem] * len(state),
        out_specs=[hbm, hbm],
        out_shape=[out, out],
        scratch_shapes=[
            pltpu.VMEM((COLS, ROWS), F32), pltpu.VMEM((COLS, ROWS), F32), pltpu.SMEM((8, N), I32), dma((9,)),
        ],
        compiler_params=pltpu.CompilerParams(vmem_limit_bytes=4 * 2**20),
        name="write",
    )(*state)


def solution(mesh):
    in_specs = (P(None, None, "rows"), P(None, "rows"))
    out_specs = (P(None, None, "rows"), P(None, None, "rows"))
    return jax.shard_map(per_device, mesh=mesh, in_specs=in_specs, out_specs=out_specs, check_vma=False)
```

```python
import jax
import jax.numpy as jnp
from jax import lax
from jax.experimental import pallas as pl
from jax.experimental.pallas import tpu as pltpu
from jax.sharding import PartitionSpec as P

SPAN = 4096
W = 128
STREAMS = 4
COLS = 32
ROWS = 8192
TILES = ROWS // W
LEAD = 8
TABLE = TILES + LEAD + 2
EARLY = SPAN + W
N = TILES * STREAMS
BASE = ((0, 3), (1, 3), (2, 3))
EXTRA = ((0, 2), (1, 2))
UNITS = BASE + EXTRA
RELAYS_MIDDLE = ((), (), ((0, 1), (3, 1)), ((1, 1), (4, 1)))
RELAYS_FIRST = ((), (), (), ((0, 2),))
RELAYS = ((), (), (), ((3, 2), (2, 1), (1, 2), (4, 2), (2, 2)))
ORDER = (0, 1, 2)
MESH = pl.DeviceIdType.MESH
F32 = jnp.float32
I32 = jnp.int32
BF16 = jnp.bfloat16


def lanes_of(shape):
    return lax.broadcasted_iota(I32, shape, len(shape) - 1)


def rows_of(shape):
    return lax.broadcasted_iota(I32, shape, 0)


def lane_gather(values, index):
    return jnp.take_along_axis(values, index, axis=1, mode="promise_in_bounds")


def dot(a, b):
    return jnp.dot(a, b, preferred_element_type=F32)


def make_weights(w_ref):
    r = rows_of(w_ref.shape) % W
    c = lanes_of(w_ref.shape)
    w_ref[...] = ((r <= c % W) | (c >= W)).astype(F32).astype(BF16)


def index_maps(keep_ref, keepi_ref, keepf_ref, src_ref, rank_ref, places_ref, moves_ref):
    for t in range(TILES):
        keepi_ref[pl.ds(STREAMS * t, STREAMS), :] = keep_ref[:, t * W : (t + 1) * W]
    keep = keepi_ref[...].astype(F32)
    keepf_ref[...] = keep
    keep = keep.astype(BF16)
    tri = (rows_of((W, W)) <= lanes_of((W, W))).astype(F32).astype(BF16)
    ones = jnp.ones((W, W), BF16)
    inside = dot(keep, tri)
    count = dot(keep, ones)
    counts = count.astype(BF16)
    ri, ci = rows_of((N, N)), lanes_of((N, N))
    same = (ri & (STREAMS - 1)) == (ci & (STREAMS - 1))
    before = (same & ((ci >> 2) < (ri >> 2))).astype(F32).astype(BF16)
    same = same.astype(F32).astype(BF16)
    turned = keepi_ref[...].T
    count_row = jnp.sum(turned, axis=0, keepdims=True)
    count_row = jnp.broadcast_to(count_row, (8, N))
    start_row = count_row
    for k in range(6):
        step = STREAMS << k
        start_row = start_row + jnp.where(lanes_of((8, N)) >= step, pltpu.roll(start_row, step, 1), 0)
    start_row = start_row - count_row
    sub = rows_of((8, N))
    first_row = jnp.broadcast_to(turned[0:1], (8, N))
    places_ref[...] = start_row + jnp.where(sub == 1, count_row, jnp.where(sub == 2, first_row, 0))
    start = dot(before, counts).astype(I32)
    total = dot(same, counts).astype(I32)
    inside = inside.astype(I32)
    rank_ref[...] = start + inside
    place = start - total + ROWS
    wanted = (lanes_of((N, W)) - place) & (W - 1)
    way = jnp.where(wanted < count.astype(I32), ((place + wanted) >> 7) - (rows_of((N, W)) >> 2), 0)
    for k in range(6):
        step = STREAMS << k
        moves = (way >> k) & 1
        moves_ref[k, STREAMS * LEAD :, :] = moves
        moves_ref[k, : STREAMS * LEAD, :] = jnp.zeros((STREAMS * LEAD, W), I32)
        arrives = pltpu.roll(moves, step, 0)
        way = jnp.where(arrives == 1, pltpu.roll(way, step, 0), jnp.where(moves == 1, 0, way))
    found = jnp.zeros((N, W), I32)
    for step in (64, 32, 16, 8, 4, 2, 1):
        probe = lane_gather(inside, found + (step - 1))
        found = jnp.where(probe <= wanted, found + step, found)
    src_ref[...] = found
    return total[0:8, :].astype(F32)


def prefixes(s, events_ref, keepf_ref, w_ref, prefix_ref, exclusive):
    group = 16

    def body(g, base):
        kept, lhs = [], []
        for u in range(group):
            t = g * group + u
            x = events_ref[:, pl.ds(pl.multiple_of(t * W, W), W)]
            x = x * keepf_ref[pl.ds(STREAMS * t + s, 1), :]
            kept.append(x)
            hi = x.astype(BF16)
            lhs.append(jnp.concatenate([hi, (x - hi.astype(F32)).astype(BF16)], axis=1))
        sums = dot(jnp.concatenate(lhs, axis=0), w_ref[...])
        for u in range(group):
            part = sums[u * COLS : (u + 1) * COLS]
            prefix = base + part[:, :W]
            base = base + part[:, W:]
            prefix_ref[g * group + u] = prefix
            exclusive[g * group + u] = prefix - kept[u]
        return base

    return lax.fori_loop(0, TILES // group, body, jnp.zeros((COLS, W), F32))


def tile_at(t):
    return pl.ds(pl.multiple_of(t * W, W), W)


def compact(s, src_ref, moves_ref, exclusive, table):
    group = 16

    def gather(g, _):
        for u in range(group):
            t = g * group + u
            index = jnp.broadcast_to(src_ref[pl.ds(STREAMS * t + s, 1), :], (COLS, W))
            table[t + LEAD] = lane_gather(exclusive[t], index)
        return 0

    lax.fori_loop(0, TILES // group, gather, 0)
    for k in range(6):
        step = 1 << k
        blocks = (TILES - step) // LEAD if step >= LEAD else TILES // LEAD

        def shift(g, _):
            moved = []
            for u in range(LEAD):
                t = TILES - 1 - g * LEAD - u
                moves = moves_ref[k, pl.ds(STREAMS * (t - step + LEAD) + s, 1), :]
                moved.append(
                    jnp.where(moves == 1, table[t - step + LEAD], table[t + LEAD])
                )
            for u in range(LEAD):
                table[TILES - 1 - g * LEAD - u + LEAD] = moved[u]
            return 0

        lax.fori_loop(0, blocks, shift, 0)


def take_tail(table, total, tail_ref):
    for t in range(SPAN // W):
        tail_ref[t] = table[LEAD + SPAN // W + t] - total


def take_early(s, at, table, windows):
    lane = lanes_of((COLS, W))
    first = ROWS - at[1, N - STREAMS + s]
    block, shift = jnp.minimum(first >> 7, SPAN // W), first & (W - 1)
    turn = (lane + shift) & (W - 1)
    fresh = lane < W - shift

    def rolled(j):
        return lane_gather(table[block + j + LEAD], turn)

    def early(g, now):
        for u in range(11):
            j = g * 11 + u
            following = rolled(j + 1)
            windows[SPAN // W + j] = jnp.where(fresh, now, following)
            now = following
        return now

    lax.fori_loop(0, EARLY // W // 11, early, rolled(0))


def finish(s, at, notes, rank_ref, prefix_ref, windows, mean_ref, deviation_ref):
    before = jnp.concatenate([notes[:, g * 4 + s : g * 4 + s + 1] for g in range(4)], axis=0)
    before = jnp.broadcast_to(before, (COLS, W))
    seen = jnp.broadcast_to(notes[0:1, 16 + s : 17 + s], (1, W))
    lane = lanes_of((COLS, W))
    group = 16

    def body(g, _):
        for u in range(group):
            t = g * group + u
            row = STREAMS * t + s
            rank = rank_ref[pl.ds(row, 1), :]
            block = at[0, row] >> 7
            index = jnp.broadcast_to(rank & (W - 1), (COLS, W))
            slots = jnp.where(lane >= at[2, row] - (block << 7), windows[block], windows[block + 1])
            earlier = lane_gather(slots, index)
            prefix = prefix_ref[t]
            mean = (prefix - earlier) * (1.0 / SPAN)
            inverse = 1.0 / jnp.maximum(seen + rank.astype(F32), 1.0)
            mean_ref[:, tile_at(t)] = mean
            deviation_ref[:, tile_at(t)] = mean - (before + prefix) * inverse
        return 0

    lax.fori_loop(0, TILES // group, body, 0)


def take_message(events, keepf_ref, totals):
    group = 4

    def body(g, sums):
        sums = list(sums)
        for u in range(group):
            t = g * group + u
            for s in range(STREAMS):
                sums[s] = sums[s] + events[s, :, tile_at(t)] * keepf_ref[pl.ds(STREAMS * t + s, 1), :]
        return tuple(sums)

    zero = jnp.zeros((COLS, W), F32)
    sums = lax.fori_loop(0, TILES // group, body, (zero,) * STREAMS)
    lane = lanes_of((8, W))
    message = jnp.zeros((8, W), F32)
    for s in range(STREAMS):
        total = jnp.sum(sums[s], axis=1, keepdims=True)
        for g in range(4):
            message = jnp.where(lane == g * 4 + s, total[g * 8 : (g + 1) * 8], message)
        message = jnp.where(lane == 16 + s, totals[s : s + 1, :], message)
    return message


def kernel(
    keep_ref, events_hbm,
    mean_ref, deviation_ref, rank_ref, places_ref, prefix3, windows3, notes_ref,
    events, w_ref, keepi_ref, keepf_ref, src_ref, moves_ref, at,
    prefix_ref, exclusive, tables, tail, windows0, windows1, windows2,
    relay, mine, half, across, plane, inside, given, send, result,
    local_sem, tail_send, tail_recv, half_sem, across_sem, plane_sem, given_sem, back_sem, scan_send,
    hop_send, hop_recv,
):
    windows = (windows0, windows1, windows2, windows3)
    prefix = [prefix_ref.at[s] for s in range(3)] + [prefix3]
    loads = [None]
    for s in range(STREAMS):
        loads.append(pltpu.make_async_copy(events_hbm.at[s], events.at[s, :, pl.ds(0, ROWS)], local_sem.at[1 + s]))
    for load in loads[1:]:
        load.start()
    devices = lax.axis_size("rows")
    me = lax.axis_index("rows")
    core, chip = me % 2, me // 2
    x, zy = chip % 4, chip // 4
    even = core == 0

    def other_x(step):
        return (zy * 4 + (x + step) % 4) * 2

    def other_plane(step):
        return (((zy + step) % 16) * 4 + x) * 2

    barrier = pltpu.get_barrier_semaphore()

    def greet(device):
        pl.semaphore_signal(barrier, inc=1, device_id=(device,), device_id_type=MESH)

    def remote(src, dst, send_sem, recv_sem, device):
        return pltpu.make_async_remote_copy(
            src_ref=src, dst_ref=dst, send_sem=send_sem, recv_sem=recv_sem,
            device_id=(device,), device_id_type=MESH,
        )

    following, preceding = (me + 1) % devices, (me + devices - 1) % devices
    ahead, behind = (zy * 4 + (x + 1) % 4) * 2, (zy * 4 + (x + 3) % 4) * 2
    next_line, last_line = ((zy + 1) % 16 * 4 + 2) * 2 + 1, ((zy + 15) % 16 * 4 + 3) * 2 + 1
    first_relay = jnp.where(x == 3, next_line, behind + 1)
    starts = (core == 1) & (me < devices - 1)
    relays = (core == 1) & ((x != 2) | (zy > 0))
    relays_on = (core == 1) & ((x != 1) | (zy > 0))

    greet(following)
    greet(preceding)

    @pl.when(even)
    def _():
        for step in range(1, 4):
            greet(other_x(step))
        greet(ahead + 1)

    @pl.when(even & (x > 0))
    def _():
        for step in range(1, 16):
            greet(other_plane(step))

    @pl.when(core == 1)
    def _():
        greet(ahead + 1)
        greet(behind + 1)
        greet(behind)

    @pl.when((core == 1) & (x == 3))
    def _():
        greet(next_line)

    @pl.when((core == 1) & (x == 2))
    def _():
        greet(last_line)

    make_weights(w_ref)
    totals = index_maps(keep_ref, keepi_ref, keepf_ref, src_ref, rank_ref, places_ref, moves_ref)
    places = pltpu.make_async_copy(places_ref, at, local_sem.at[5])
    places.start()

    def everyone_is_here():
        @pl.when(even & (x == 0))
        def _():
            pl.semaphore_wait(barrier, 6)

        @pl.when(even & (x > 0))
        def _():
            pl.semaphore_wait(barrier, 21)

        @pl.when((core == 1) & (x < 2))
        def _():
            pl.semaphore_wait(barrier, 5)

        @pl.when((core == 1) & (x >= 2))
        def _():
            pl.semaphore_wait(barrier, 6)

    def whole_copy(s):
        return remote(
            tail.at[s], windows[s].at[pl.ds(0, SPAN // W)], tail_send.at[s], tail_recv.at[s], following
        )

    def units_of(s, extra):
        return [u for u in range(len(UNITS)) if UNITS[u][0] == s and (extra or u < len(BASE))]

    def part_copy(s, extra):
        part = pl.ds(0, COLS - 8 * len(units_of(s, extra)))
        return remote(
            tail.at[s, :, part], windows[s].at[pl.ds(0, SPAN // W), part],
            tail_send.at[s], tail_recv.at[s], following,
        )

    def hop(unit, k):
        s, group = UNITS[unit]
        part = pl.ds(8 * group, 8)
        src = tail.at[s, :, part] if k == 0 else relay.at[k - 1, unit]
        dst = windows[s].at[pl.ds(0, SPAN // W), part] if k == 2 else relay.at[k, unit]
        device = (first_relay, behind + 1, behind)[k]
        return remote(src, dst, hop_send.at[k, unit], hop_recv.at[k, unit], device)

    def pass_on(unit, k):
        here = (relays, relays_on)[k - 1]
        if unit >= len(BASE):
            here = here & (x == 3 - k)

        @pl.when(here)
        def _():
            hop(unit, k - 1).wait_recv()
            hop(unit, k).start()

    def across_copy(k):
        return remote(across.at[0], across.at[k], scan_send.at[k], across_sem.at[k], other_x(k))

    def plane_copy(k):
        return remote(plane.at[0], plane.at[k], scan_send.at[3 + k], plane_sem.at[k], other_plane(k))

    up = remote(mine, half, scan_send.at[0], half_sem, preceding)
    back = remote(send, result, scan_send.at[0], back_sem, following)
    lines_copy = remote(given, result, scan_send.at[19], given_sem, behind)

    def scan_step(step):
        if step == 0:
            mine[...] = take_message(events, keepf_ref, totals)

            @pl.when(core == 1)
            def _():
                up.start()

        if step == 1:

            @pl.when(even)
            def _():
                up.wait_recv()
                across[0] = mine[...] + half[...]
                for k in range(1, 4):
                    across_copy(k).start()

        if step == 2:

            @pl.when(even & (x > 0))
            def _():
                group = across[0]
                before = jnp.zeros((8, W), F32)
                for k in range(1, 4):
                    across_copy(k).wait_recv()
                    piece = across[k]
                    group = group + piece
                    before = before + jnp.where((x + 4 - k) % 4 < x, piece, 0.0)
                inside[...] = before
                plane[0] = group
                for k in range(1, 16):
                    plane_copy(k).start()

        if step == 3:

            @pl.when(even & (x > 0))
            def _():
                lines = jnp.zeros((8, W), F32)
                for k in range(1, 16):
                    plane_copy(k).wait_recv()
                    lines = lines + jnp.where((zy + 16 - k) % 16 < zy, plane[k], 0.0)
                given[...] = lines
                result[...] = inside[...] + lines

            @pl.when(even & (x == 1))
            def _():
                lines_copy.start()

            @pl.when(even & (x > 0))
            def _():
                send[...] = result[...] + mine[...]
                back.start()

        if step == 4:

            @pl.when(even & (x == 0))
            def _():
                for k in range(1, 4):
                    across_copy(k).wait_recv()
                lines_copy.wait_recv()
                send[...] = result[...] + mine[...]
                back.start()

            @pl.when(core == 1)
            def _():
                back.wait_recv()

    for s in range(STREAMS):
        table = tables.at[s % 2]
        if s == 0:
            loads[1].wait()
        total = prefixes(s, events.at[s], keepf_ref, w_ref, prefix[s], exclusive)
        for unit, k in RELAYS_MIDDLE[s]:
            pass_on(unit, k)
        if s == 1:
            scan_step(1)
        if s == 3:
            scan_step(3)
        compact(s, src_ref, moves_ref, exclusive, table)
        take_tail(table, total, tail.at[s])
        if s == 0:
            everyone_is_here()
        for unit, k in RELAYS_FIRST[s]:
            pass_on(unit, k)

        @pl.when(even)
        def _():
            whole_copy(s).start()

        for extra in (False, True):

            @pl.when(starts & ((x == 3) == extra))
            def _():
                part_copy(s, extra).start()
                for unit in units_of(s, extra):
                    hop(unit, 0).start()

        if s == 0:
            for load in loads[2:]:
                load.wait()
            places.wait()
            scan_step(0)
        if s == 1:
            scan_step(2)
        if s > 0:
            take_early(s - 1, at, tables.at[(s - 1) % 2], windows[s - 1])
        for unit, k in RELAYS[s]:
            pass_on(unit, k)
    take_early(STREAMS - 1, at, tables.at[(STREAMS - 1) % 2], windows[STREAMS - 1])
    scan_step(4)
    notes = result[...]

    @pl.when(me == 0)
    def _():
        for s in range(STREAMS):
            for t in range(SPAN // W):
                windows[s][t] = jnp.zeros((COLS, W), F32)

    notes_ref[...] = notes

    def wait_tail(s):
        @pl.when(core == 1)
        def _():
            whole_copy(s).wait_recv()

        for extra in (False, True):

            @pl.when(even & (me > 0) & ((x == 0) == extra))
            def _():
                part_copy(s, extra).wait_recv()
                for unit in units_of(s, extra):
                    hop(unit, 2).wait_recv()

    for s in ORDER:
        wait_tail(s)
        finish(s, at, notes, rank_ref, prefix[s], windows[s], mean_ref.at[s], deviation_ref.at[s])
    wait_tail(3)

    @pl.when(even)
    def _():
        for s in range(STREAMS):
            whole_copy(s).wait_send()
        for k in range(1, 4):
            across_copy(k).wait_send()
        back.wait_send()

    @pl.when(core == 1)
    def _():
        up.wait_send()

    @pl.when(even & (x > 0))
    def _():
        for k in range(1, 16):
            plane_copy(k).wait_send()

    @pl.when(even & (x == 1))
    def _():
        lines_copy.wait_send()

    for extra in (False, True):

        @pl.when(starts & ((x == 3) == extra))
        def _():
            for s in range(STREAMS):
                part_copy(s, extra).wait_send()
                for unit in units_of(s, extra):
                    hop(unit, 0).wait_send()

    for k, sender in ((1, relays), (2, relays_on)):

        @pl.when(sender)
        def _():
            for unit in range(len(BASE)):
                hop(unit, k).wait_send()

        @pl.when(sender & (x == 3 - k))
        def _():
            for unit in range(len(BASE), len(UNITS)):
                hop(unit, k).wait_send()


def write_kernel(
    mean_ref, deviation_ref, rank_ref, places_ref, prefix_ref, windows, notes_ref,
    mean_hbm, deviation_hbm,
    mean, deviation, at, sems,
):
    places = pltpu.make_async_copy(places_ref, at, sems.at[0])
    places.start()
    copies = []
    for s in range(3):
        copies.append(pltpu.make_async_copy(mean_ref.at[s], mean_hbm.at[s], sems.at[2 * s + 1]))
        copies.append(pltpu.make_async_copy(deviation_ref.at[s], deviation_hbm.at[s], sems.at[2 * s + 2]))
    for copy in copies:
        copy.start()
    places.wait()
    finish(3, at, notes_ref[...], rank_ref, prefix_ref, windows, mean, deviation)
    copies.append(pltpu.make_async_copy(mean, mean_hbm.at[3], sems.at[7]))
    copies.append(pltpu.make_async_copy(deviation, deviation_hbm.at[3], sems.at[8]))
    for copy in copies[-2:]:
        copy.start()
    for copy in copies:
        copy.wait()


def per_device(events, keep):
    out = jax.ShapeDtypeStruct((STREAMS, COLS, ROWS), F32)
    tile = pltpu.VMEM((8, W), F32)
    dma = pltpu.SemaphoreType.DMA
    hbm = pl.BlockSpec(memory_space=pltpu.HBM)
    vmem = pl.BlockSpec(memory_space=pltpu.VMEM)
    three = jax.ShapeDtypeStruct((3, COLS, ROWS), F32)
    state = [
        three, three,
        jax.ShapeDtypeStruct((N, W), I32),
        jax.ShapeDtypeStruct((8, N), I32),
        jax.ShapeDtypeStruct((TILES, COLS, W), F32),
        jax.ShapeDtypeStruct((TILES + 3, COLS, W), F32),
        jax.ShapeDtypeStruct((8, W), F32),
    ]
    state = pl.pallas_call(
        kernel,
        in_specs=[vmem, hbm],
        out_specs=[vmem] * len(state),
        out_shape=state,
        scratch_shapes=[
            pltpu.VMEM((STREAMS, COLS, ROWS + W), F32),
            pltpu.VMEM((2 * W, 2 * W), BF16),
            pltpu.VMEM((N, W), I32),
            pltpu.VMEM((N, W), F32),
            pltpu.VMEM((N, W), I32),
            pltpu.VMEM((6, N + STREAMS * LEAD, W), I32),
            pltpu.SMEM((8, N), I32),
            pltpu.VMEM((3, TILES, COLS, W), F32),
            pltpu.VMEM((TILES, COLS, W), F32),
            pltpu.VMEM((2, TABLE, COLS, W), F32),
            pltpu.VMEM((STREAMS, SPAN // W, COLS, W), F32),
        ]
        + [pltpu.VMEM((TILES + 3, COLS, W), F32)] * 3
        + [
            pltpu.VMEM((2, len(UNITS), SPAN // W, 8, W), F32),
            tile, tile, pltpu.VMEM((4, 8, W), F32), pltpu.VMEM((16, 8, W), F32), tile, tile, tile, tile,
            dma((6,)), dma((STREAMS,)), dma((STREAMS,)), dma, dma((4,)), dma((16,)), dma, dma, dma((20,)),
            dma((3, len(UNITS))), dma((3, len(UNITS))),
        ],
        compiler_params=pltpu.CompilerParams(
            collective_id=0, has_side_effects=True, vmem_limit_bytes=43 * 2**20
        ),
        name="windows",
    )(keep, events)
    return pl.pallas_call(
        write_kernel,
        in_specs=[vmem] * len(state),
        out_specs=[hbm, hbm],
        out_shape=[out, out],
        scratch_shapes=[
            pltpu.VMEM((COLS, ROWS), F32), pltpu.VMEM((COLS, ROWS), F32), pltpu.SMEM((8, N), I32), dma((9,)),
        ],
        compiler_params=pltpu.CompilerParams(vmem_limit_bytes=4 * 2**20),
        name="write",
    )(*state)


def solution(mesh):
    in_specs = (P(None, None, "rows"), P(None, "rows"))
    out_specs = (P(None, None, "rows"), P(None, None, "rows"))
    return jax.shard_map(per_device, mesh=mesh, in_specs=in_specs, out_specs=out_specs, check_vma=False)
```
